256 devices in a mesh: dp: 8 (over x, core), mp: 32 (over y, z).
Axes of the slice: x: 4, y: 4, z: 8, core: 2. Of those that a mesh axis runs over, the one named last changes fastest.
Arguments:
- hidden: bfloat16 [8, 4, 512, 2048], P('dp', None, None, 'mp'), may hold values from -6 to 6
- gain: float32 [2048], P('mp'), may hold values from 0.1 to 1.9
- cotangent: bfloat16 [8, 4, 512, 2048], P('dp', None, None, 'mp'), may hold values from -600 to 600
- blocks: int32 [8, 4, 2], P('dp'), may hold values from 1 to 2
- loss_mask: int32 [8, 4, 512], P('dp'), may hold values 0 or 1
- wi_gate: bfloat16 [5120, 2048], P('mp'), may hold values from -0.125 to 0.125
- wi_up: bfloat16 [5120, 2048], P('mp'), may hold values from -0.125 to 0.125
- wo_weight: bfloat16 [5120, 2048], P('mp'), may hold values from -0.078125 to 0.078125
Outputs:
- gradients: float32 [3, 5120, 2048], P(None, 'mp')
The draws below stay inside these ranges and needn't reach their ends.
Inputs may be any that keep to these rules, and one draw needn't show every extreme that they name: blocks of 128 target positions used by a sequence; later positions are padding.
All inputs are finite; a program needn't handle non-finite values. No bound on the sum of `loss_mask` on one device may be relied on, other than what follows from the above.
Results may differ from the reference program's by a relative error of at most 0.0059.
Values may be sent and summed in bfloat16 or wider, within the bound.
No kernel may reach another device: no remote copies, remote signals or barrier semaphores. Data moves between devices by JAX's collectives and lax.ppermute only.
A program may use at most 128 MiB of HBM per device.

```python
import jax
import jax.numpy as jnp
from jax import lax

D = 2048
FF = 5120
MICRO = 4
BLOCK = 128
NBLK = 2
SEQ_MB = 2
GROUPS = 8
TLEN = 256
TOK_MB = 512


def place_ends(drawn, rng, low, high):
    extent = drawn.shape
    place = [jax.random.randint(jax.random.fold_in(rng, axis), (), 0, extent[axis]) for axis in range(len(extent))]
    drawn = drawn.at[tuple(place)].set(low)
    longest = extent.index(max(extent))
    place[longest] = (place[longest] + 1) % extent[longest]
    return drawn.at[tuple(place)].set(high)


def shard_levels(key, shape, pieces, least, top_value):
    def one(dim, shards_of):
        heights = jax.random.uniform(jax.random.fold_in(jax.random.fold_in(key, 6), dim), (shards_of,), jnp.float32, least / len(pieces), top_value / len(pieces))
        return jnp.repeat(jnp.exp(heights), shape[dim] // shards_of).reshape((-1,) + (1,) * (len(shape) - dim - 1))

    loudness = one(*pieces[0])
    for cut in pieces[1:]:
        loudness = loudness * one(*cut)
    return loudness


def normal_values(own_key, extent, width, reach, cuts=(), kind=jnp.bfloat16):
    values = width * jax.random.normal(own_key, extent, jnp.float32)
    if cuts:
        values = values * shard_levels(own_key, extent, cuts, -0.22, 0.18)
    return jnp.clip(values, -reach, reach).astype(kind)


def setup_inputs(seed: int = 0) -> dict:
    seeds = jax.random.split(jax.random.key(seed), 9)
    return {
        "hidden": normal_values(seeds[0], (GROUPS, MICRO, TOK_MB, D), 1.0, 6.0, ((0, 8), (3, 32))),
        "gain": jnp.clip(1.0 + 0.18 * jax.random.normal(seeds[1], (D,), jnp.float32), 0.1, 1.9),
        "cotangent": normal_values(seeds[2], (GROUPS, MICRO, TOK_MB, D), 100.0, 600.0, ((0, 8), (3, 32))),
        "blocks": place_ends(jax.random.randint(seeds[3], (GROUPS, MICRO, SEQ_MB), 1, NBLK + 1), jax.random.fold_in(seeds[3], 1), 1, NBLK).astype(jnp.int32),
        "loss_mask": place_ends((jax.random.randint(seeds[4], (GROUPS, MICRO, TOK_MB), 0, 4) < 3).astype(jnp.int32), jax.random.fold_in(seeds[4], 1), 0, 1),
        "wi_gate": normal_values(seeds[5], (FF, D), D ** -0.5, 0.125, ((0, 32),)),
        "wi_up": normal_values(seeds[6], (FF, D), D ** -0.5, 0.125, ((0, 32),)),
        "wo_weight": normal_values(seeds[7], (FF, D), FF ** -0.5, 0.078125, ((0, 32),)),
    }


def gelu_tanh(value):
    return jax.nn.gelu(value, approximate=True)

def contributions(normed, tangent, wi_gate, wi_up, wo_weight):
    rows_dims = (((1,), (1,)), ((), ()))
    gate_pre = lax.dot_general(normed, wi_gate, rows_dims, preferred_element_type=jnp.float32)
    up_pre = lax.dot_general(normed, wi_up, rows_dims, preferred_element_type=jnp.float32)
    activated, pullback = jax.vjp(gelu_tanh, gate_pre)
    inner = (activated * up_pre).astype(jnp.bfloat16)
    back_grad = lax.dot_general(tangent, wo_weight, rows_dims, preferred_element_type=jnp.float32)
    grad_gate = pullback(back_grad * up_pre)[0].astype(jnp.bfloat16)
    grad_up = (back_grad * activated).astype(jnp.bfloat16)
    dims = (((0,), (0,)), ((), ()))
    first_grad = lax.dot_general(grad_gate, normed, dims, preferred_element_type=jnp.float32)
    second_grad = lax.dot_general(grad_up, normed, dims, preferred_element_type=jnp.float32)
    third_grad = lax.dot_general(inner, tangent, dims, preferred_element_type=jnp.float32)
    return jnp.stack([first_grad, second_grad, third_grad])

def reference(hidden, gain, cotangent, blocks, loss_mask, wi_gate, wi_up, wo_weight):
    position = jnp.arange(TOK_MB, dtype=jnp.int32)
    offset = position % TLEN
    sequence = position // TLEN
    limit_pos = blocks[:, :, sequence] * BLOCK
    weight = (offset[None, None, :] < limit_pos).astype(jnp.int32) * loss_mask
    token_total = jnp.sum(weight)
    states = hidden.astype(jnp.float32)
    normed = (states * lax.rsqrt(lax.optimization_barrier(jnp.mean(states * states, axis=-1, keepdims=True)) + 1e-06) * gain).astype(jnp.bfloat16)
    tangent = cotangent * weight[..., None].astype(jnp.bfloat16)
    overall = jnp.zeros((3, FF, D), jnp.float32)
    for group_index in range(GROUPS):
        running_sum = jnp.zeros((3, FF, D), jnp.float32)
        compensation = jnp.zeros((3, FF, D), jnp.float32)
        for micro_step in range(MICRO):
            contrib = contributions(normed[group_index, micro_step], tangent[group_index, micro_step], wi_gate, wi_up, wo_weight)
            adjusted = contrib - compensation
            running = running_sum + adjusted
            compensation = running - running_sum - adjusted
            running_sum = running
        overall = overall + running_sum
    return overall / jnp.maximum(token_total, 1).astype(jnp.float32)
```

```python
import jax
import jax.numpy as jnp
from jax import lax
from jax.sharding import PartitionSpec as P

D = 2048
BLOCK = 128
TLEN = 256


def sent_to_all(x, axis):
    devices = lax.axis_size(axis)
    return lax.all_to_all(jnp.broadcast_to(x[None], (devices, *x.shape)), axis, 0, 0, tiled=True)


def in_blocks(x, dim, devices):
    lengths = x.shape
    blocks = x.reshape(*lengths[:dim], devices, lengths[dim] // devices, *lengths[dim + 1 :])
    return jnp.moveaxis(blocks, dim, 0)


def summed_on_arrival(x, axis, dim):
    blocks = in_blocks(x, dim, lax.axis_size(axis))
    arrived = lax.all_to_all(blocks, axis, split_axis=0, concat_axis=0, tiled=True)
    return arrived.astype(jnp.float32).sum(axis=0)


def gelu_tanh(value):
    return jax.nn.gelu(value, approximate=True)


def contributions(normed, tangent, wi_gate, wi_up, wo_weight):
    rows_dims = (((1,), (0,)), ((), ()))
    gate_pre = lax.dot_general(wi_gate, normed, rows_dims, preferred_element_type=jnp.float32)
    up_pre = lax.dot_general(wi_up, normed, rows_dims, preferred_element_type=jnp.float32)
    activated, pullback = jax.vjp(gelu_tanh, gate_pre)
    inner = (activated * up_pre).astype(jnp.bfloat16)
    back_grad = lax.dot_general(wo_weight, tangent, rows_dims, preferred_element_type=jnp.float32)
    grad_gate = pullback(back_grad * up_pre)[0].astype(jnp.bfloat16)
    grad_up = (back_grad * activated).astype(jnp.bfloat16)
    dims = (((1,), (1,)), ((), ()))
    first_grad = lax.dot_general(grad_gate, normed, dims, preferred_element_type=jnp.float32)
    second_grad = lax.dot_general(grad_up, normed, dims, preferred_element_type=jnp.float32)
    third_grad = lax.dot_general(inner, tangent, dims, preferred_element_type=jnp.float32)
    return first_grad, second_grad, third_grad


def on_device(hidden, gain, cotangent, blocks, loss_mask, wi_gate, wi_up, wo_weight):
    row_count = hidden.shape[2]
    micro_count = hidden.shape[1]
    own = jnp.concatenate(
        [jnp.moveaxis(a[0], 2, 0).reshape(a.shape[3], -1) for a in (hidden, cotangent)], axis=1
    )
    whole = lax.all_gather(own, "mp", axis=0, tiled=True)
    whole_gain = sent_to_all(gain, "mp").reshape(-1, 1)
    position = lax.iota(jnp.int32, row_count)
    offset = position % TLEN
    sequence = position // TLEN
    picker = (sequence[None, :] == lax.iota(jnp.int32, blocks.shape[2])[:, None]).astype(jnp.int32)
    limit_pos = jnp.sum(blocks[0][:, :, None] * picker[None, :, :], axis=1) * BLOCK
    weight = (offset[None, :] < limit_pos).astype(jnp.int32) * loss_mask[0]
    token_total = sent_to_all(jnp.sum(weight), "dp").sum(axis=0)
    denominator = jnp.maximum(token_total, 1).astype(jnp.float32)
    totals = [jnp.zeros(wi_gate.shape, jnp.float32)] * 3
    comps = totals
    for micro_step in range(micro_count):
        start = micro_step * row_count
        states = whole[:, start : start + row_count].astype(jnp.float32)
        squares = jnp.sum(states * states, axis=0, keepdims=True)
        normed = (states * lax.rsqrt(squares / D + 1e-06) * whole_gain).astype(jnp.bfloat16)
        start += micro_count * row_count
        tangent = whole[:, start : start + row_count] * weight[micro_step][None].astype(jnp.bfloat16)
        terms = contributions(normed, tangent, wi_gate, wi_up, wo_weight)
        adjusted = [term - comp for term, comp in zip(terms, comps)]
        running = [total + a for total, a in zip(totals, adjusted)]
        comps = [r - total - a for r, total, a in zip(running, totals, adjusted)]
        totals = running
    running_sum = jnp.stack([total.astype(jnp.bfloat16) for total in totals])
    share_part = summed_on_arrival(running_sum, "dp", 2)
    share_part = share_part / denominator
    result = lax.all_gather(share_part.astype(jnp.bfloat16), "dp", axis=2, tiled=True).astype(
        share_part.dtype
    )
    return result


def solution(mesh):
    return jax.shard_map(
        on_device,
        mesh=mesh,
        in_specs=(
            P("dp", None, None, "mp"),
            P("mp"),
            P("dp", None, None, "mp"),
            P("dp", None, None),
            P("dp", None, None),
            P("mp", None),
            P("mp", None),
            P("mp", None),
        ),
        out_specs=P(None, "mp", None),
        check_vma=False,
    )
```

```python
import functools

import jax
import jax.numpy as jnp
from jax import lax
from jax.experimental import pallas as pl
from jax.experimental.pallas import tpu as pltpu
from jax.sharding import Mesh
from jax.sharding import PartitionSpec as P

D = 2048
BLOCK = 128
TLEN = 256
DP = ("x", "core")
MP = ("y", "z")
NY = 4
NZ = 8
CHUNK = 512
GROUPS_Z = ((0, 1, 7), (2, 6, 3, 5, 4))


def sent_to_all(x, axis):
    devices = lax.axis_size(axis)
    return lax.all_to_all(jnp.broadcast_to(x[None], (devices, *x.shape)), axis, 0, 0, tiled=True)


def in_blocks(x, dim, devices):
    lengths = x.shape
    blocks = x.reshape(*lengths[:dim], devices, lengths[dim] // devices, *lengths[dim + 1 :])
    return jnp.moveaxis(blocks, dim, 0)


def summed_on_arrival(x, axis, dim):
    blocks = in_blocks(x, dim, lax.axis_size(axis))
    arrived = lax.all_to_all(blocks, axis, split_axis=0, concat_axis=0, tiled=True)
    return arrived.astype(jnp.float32).sum(axis=0)


def shifted(x, axis, step):
    size = lax.axis_size(axis)
    return lax.ppermute(x, axis, [(i, (i + step) % size) for i in range(size)])


def ring(own, axis):
    size = lax.axis_size(axis)
    ahead, behind = own, own
    blocks = {0: own}
    for step in range(1, size // 2):
        ahead, behind = shifted(ahead, axis, 1), shifted(behind, axis, -1)
        blocks[step], blocks[size - step] = ahead, behind
    blocks[size // 2] = (shifted(ahead[0], axis, 1), shifted(behind[1], axis, -1))
    return blocks


def joined(blocks, order):
    return jnp.stack([jnp.stack(b) if isinstance(b, tuple) else b for b in (blocks[k] for k in order)], axis=1)


def gathered(own, first):
    part_a, part_b = own[:, :, :first], own[:, :, first:]
    pieces = []
    rows_b = ring(part_b, "z")
    column_a = ring(part_a, "y")
    joined_a = joined(column_a, range(NY))
    for back_z, got in ring(joined_a, "z").items():
        pieces.append((got, [(k, back_z) for k in range(NY)], 0))
    for group in GROUPS_Z:
        for back_y, got in ring(joined(rows_b, group), "y").items():
            pieces.append((got, [(back_y, k) for k in group], first))
    return pieces


def gradients_kernel(plan, count, place_ref, *refs):
    pieces = refs[: len(plan)]
    gain_ref, gate_ref, up_ref, down_ref, out_ref = refs[len(plan) : len(plan) + 5]
    normed, tangent, squares, scale, d_gate, d_up, inner = refs[len(plan) + 5 :]
    place_y, place_z = place_ref[0], place_ref[1]
    feats = 64

    def row_of(back_y, back_z):
        row_y = lax.rem(place_y + (NY - back_y), NY)
        row_z = lax.rem(place_z + (NZ - back_z), NZ)
        return pl.multiple_of((row_y * NZ + row_z) * feats, feats)

    squares[...] = jnp.zeros_like(squares)
    for ref, (tensors, blocks, base, length) in zip(pieces, plan):
        if 0 not in tensors:
            continue
        for k in range(len(blocks)):
            @pl.loop(0, length // 128)
            def _(tile, ref=ref, k=k, base=base, many=len(tensors) > 1):
                lanes = pl.ds(pl.multiple_of(tile * 128, 128), 128)
                states = (ref[0, k, :, lanes] if many else ref[k, :, lanes]).astype(jnp.float32)
                into = pl.ds(pl.multiple_of(base + tile * 128, 128), 128)
                squares[:, into] += (states * states).reshape(feats // 8, 8, 128).sum(axis=0)

    @pl.loop(0, count // 128)
    def _(tile):
        lanes = pl.ds(pl.multiple_of(tile * 128, 128), 128)
        mean = jnp.sum(squares[:, lanes], axis=0, keepdims=True) / D
        scale[:, lanes] = jnp.broadcast_to(lax.rsqrt(mean + 1e-06), (8, 128))

    for ref, (tensors, blocks, base, length) in zip(pieces, plan):
        many = len(tensors) > 1
        for k, back in enumerate(blocks):
            rows = pl.ds(row_of(*back), feats)
            for tensor in tensors:
                @pl.loop(0, length // 128)
                def _(tile, ref=ref, k=k, base=base, many=many, tensor=tensor, rows=rows):
                    lanes = pl.ds(pl.multiple_of(tile * 128, 128), 128)
                    into = pl.ds(pl.multiple_of(base + tile * 128, 128), 128)
                    values = ref[tensor, k, :, lanes] if many else ref[k, :, lanes]
                    if tensor:
                        tangent[rows, into] = values
                    else:
                        by = scale[0:1, into]
                        normed[rows, into] = (values.astype(jnp.float32) * by * gain_ref[rows, :]).astype(jnp.bfloat16)

    def forward(lanes):
        dims = (((1,), (0,)), ((), ()))
        x = normed[:, lanes]
        gate_pre = lax.dot_general(gate_ref[...], x, dims, preferred_element_type=jnp.float32)
        up_pre = lax.dot_general(up_ref[...], x, dims, preferred_element_type=jnp.float32)
        back = lax.dot_general(down_ref[...], tangent[:, lanes], dims, preferred_element_type=jnp.float32)
        root = 0.7978845608028654
        square = gate_pre * gate_pre
        bent = jnp.tanh(root * gate_pre * (1.0 + 0.044715 * square))
        half = 0.5 * (1.0 + bent)
        activated = gate_pre * half
        slope = half + 0.5 * gate_pre * (1.0 - bent * bent) * root * (1.0 + 3 * 0.044715 * square)
        inner[:, lanes] = (activated * up_pre).astype(jnp.bfloat16)
        d_gate[:, lanes] = (back * up_pre * slope).astype(jnp.bfloat16)
        d_up[:, lanes] = (back * activated).astype(jnp.bfloat16)

    wide = 256

    @pl.loop(0, count // wide)
    def _(tile):
        forward(pl.ds(pl.multiple_of(tile * wide, wide), wide))

    if count % wide:
        forward(pl.ds(count - count % wide, count % wide))

    spans = [(start, min(CHUNK, count - start)) for start in range(0, count, CHUNK)]
    for index, (left, right) in enumerate(((d_gate, normed), (d_up, normed), (inner, tangent))):
        @pl.loop(0, D // wide)
        def _(tile, index=index, left=left, right=right):
            rows = pl.ds(pl.multiple_of(tile * wide, wide), wide)
            total = comp = None
            for start, size in spans:
                term = lax.dot_general(
                    left[:, start : start + size],
                    right[rows, start : start + size],
                    (((1,), (1,)), ((), ())),
                    preferred_element_type=jnp.float32,
                )
                if total is None:
                    total, comp = term, jnp.zeros_like(term)
                    continue
                adjusted = term - comp
                running = total + adjusted
                comp = (running - total) - adjusted
                total = running
            out_ref[index, :, rows] = total.astype(jnp.bfloat16)


def gradients(pieces, place, gain, wi_gate, wi_up, wo_weight, count):
    plan, arrays = [], []
    for got, blocks, base in pieces:
        both = got if isinstance(got, tuple) else (got,)
        for tensor, array in enumerate(both):
            tensors = (tensor,) if isinstance(got, tuple) else (0, 1)
            plan.append((tensors, blocks, base, array.shape[-1]))
            arrays.append(array)
    units = wi_gate.shape[0]
    in_vmem = pl.BlockSpec(memory_space=pltpu.VMEM)
    return pl.pallas_call(
        functools.partial(gradients_kernel, plan, count),
        out_shape=jax.ShapeDtypeStruct((3, units, D), jnp.bfloat16),
        in_specs=[pl.BlockSpec(memory_space=pltpu.SMEM)] + [in_vmem] * (len(arrays) + 4),
        out_specs=in_vmem,
        scratch_shapes=[
            pltpu.VMEM((D, count), jnp.bfloat16),
            pltpu.VMEM((D, count), jnp.bfloat16),
            pltpu.VMEM((8, count), jnp.float32),
            pltpu.VMEM((8, count), jnp.float32),
            pltpu.VMEM((units, count), jnp.bfloat16),
            pltpu.VMEM((units, count), jnp.bfloat16),
            pltpu.VMEM((units, count), jnp.bfloat16),
        ],
        compiler_params=pltpu.CompilerParams(vmem_limit_bytes=60_000_000),
        cost_estimate=pl.CostEstimate(
            flops=12 * units * D * count, bytes_accessed=8 * D * count, transcendentals=units * count
        ),
        name="gradients",
    )(place, *arrays, gain, wi_gate, wi_up, wo_weight)


def on_device(hidden, gain, cotangent, blocks, loss_mask, wi_gate, wi_up, wo_weight):
    row_count = hidden.shape[2]
    count = hidden.shape[1] * row_count
    feats = hidden.shape[3]
    position = lax.iota(jnp.int32, row_count)
    offset = position % TLEN
    sequence = position // TLEN
    picker = (sequence[None, :] == lax.iota(jnp.int32, blocks.shape[2])[:, None]).astype(jnp.int32)
    limit_pos = jnp.sum(blocks[0][:, :, None] * picker[None, :, :], axis=1) * BLOCK
    weight = (offset[None, :] < limit_pos).astype(jnp.int32) * loss_mask[0]
    tangent = cotangent[0] * weight[:, :, None].astype(jnp.bfloat16)
    own = jnp.stack([jnp.moveaxis(a, 2, 0).reshape(feats, count) for a in (hidden[0], tangent)])
    pieces = gathered(own, 128 * round(count * 0.41 / 128))
    whole_gain = sent_to_all(gain, MP).reshape(-1, 1)
    token_total = sent_to_all(jnp.sum(weight), DP).sum(axis=0)
    denominator = jnp.maximum(token_total, 1).astype(jnp.float32)
    place = jnp.stack([lax.axis_index("y"), lax.axis_index("z")]).astype(jnp.int32)
    running_sum = gradients(pieces, place, whole_gain, wi_gate, wi_up, wo_weight, count)
    share_part = summed_on_arrival(running_sum, DP, 2)
    share_part = share_part / denominator
    result = lax.all_gather(share_part.astype(jnp.bfloat16), DP, axis=2, tiled=True).astype(
        share_part.dtype
    )
    return result


def solution(mesh):
    torus = Mesh(mesh.devices.reshape(4, 2, NY, NZ), ("x", "core", "y", "z"))
    return jax.shard_map(
        on_device,
        mesh=torus,
        in_specs=(
            P(DP, None, None, MP),
            P(MP),
            P(DP, None, None, MP),
            P(DP, None, None),
            P(DP, None, None),
            P(MP, None),
            P(MP, None),
            P(MP, None),
        ),
        out_specs=P(None, MP, None),
        check_vma=False,
    )
```

```python
import functools

import jax
import jax.numpy as jnp
from jax import lax
from jax.experimental import pallas as pl
from jax.experimental.pallas import tpu as pltpu
from jax.sharding import Mesh
from jax.sharding import PartitionSpec as P


D = 2048
BLOCK = 128
TLEN = 256
DP = ("x", "core")
MP = ("y", "z")
NY = 4
NZ = 8
CHUNK = 512
SHARE = 256
NX = 4
GROUPS_Z = ((7, 3), (2, 5))


def sent_to_all(x, axis):
    devices = lax.axis_size(axis)
    return lax.all_to_all(jnp.broadcast_to(x[None], (devices, *x.shape)), axis, 0, 0, tiled=True)


def shifted(x, axis, step):
    size = lax.axis_size(axis)
    return lax.ppermute(x, axis, [(i, (i + step) % size) for i in range(size)])


def ring(own, axis, tensor_dim):
    size = lax.axis_size(axis)
    ahead, behind = own, own
    blocks = {0: own}
    for step in range(1, size // 2):
        ahead = shifted(ahead, axis, 1)
        behind = shifted(behind, axis, -1)
        blocks[step], blocks[size - step] = ahead, behind
    first = lax.index_in_dim(ahead, 0, tensor_dim, keepdims=False)
    second = lax.index_in_dim(behind, 1, tensor_dim, keepdims=False)
    last = size // 2
    blocks[last] = (shifted(first, axis, 1), shifted(second, axis, -1))
    return blocks


def joined(blocks, order):
    return jnp.stack([jnp.stack(b) if isinstance(b, tuple) else b for b in (blocks[k] for k in order)])


def gathered(own, first):
    part_a, part_b = own[:, :, :first], own[:, :, first:]
    pieces = []

    def add(got, *where):
        if isinstance(got, tuple):
            for tensor, array in enumerate(got):
                pieces.append((array, (tensor,), *where))
        else:
            pieces.append((got, (0, 1), *where))

    rows_b = ring(part_b, "z", 0)
    column_a = ring(part_a, "y", 0)
    joined_a = joined(column_a, range(NY))
    for back_z, got in ring(joined_a, "z", 1).items():
        add(got, 0, back_z, True, 0)
    for least, many in GROUPS_Z:
        group = joined(rows_b, [(least + k) % NZ for k in range(many)])
        for back_y, got in ring(group, "y", 1).items():
            add(got, back_y, least, False, first)
    return pieces


def gradients_kernel(plan, count, place_ref, gain_ref, in_ref, down_ref, *refs):
    pieces, out_ref = refs[: len(plan)], refs[len(plan)]
    states, tangent, d_in, inner, sems = refs[len(plan) + 1 :]
    place_y, place_z = place_ref[0], place_ref[1]
    feats, units = D // (NY * NZ), down_ref.shape[0]

    def rows_of(back_y, back_z):
        row_y = lax.rem(place_y + NY - back_y, NY)
        row_z = lax.rem(place_z + NZ - back_z, NZ)
        return pl.ds(pl.multiple_of((row_y * NZ + row_z) * feats, feats), feats)

    copies = ([], [])
    for tensor, whole in enumerate((states, tangent)):
        for ref, (tensors, back_y, back_z, along_y, base) in zip(pieces, plan):
            if tensor not in tensors:
                continue
            for k in range(ref.shape[0]):
                rows = rows_of(k, back_z) if along_y else rows_of(back_y, (back_z + k) % NZ)
                copies[tensor].append(
                    pltpu.make_async_copy(
                        ref.at[k, tensor] if len(tensors) > 1 else ref.at[k],
                        whole.at[rows, pl.ds(base, ref.shape[-1])],
                        sems.at[tensor],
                    )
                )
                copies[tensor][-1].start()
    for both in copies:
        for copy in both:
            copy.wait()

    def forward(lanes):
        dims = (((1,), (0,)), ((), ()))
        x = states[:, lanes]
        wide_x = x.astype(jnp.float32)
        mean = jnp.sum(wide_x * wide_x, axis=0, keepdims=True) / D
        scale = lax.rsqrt(mean + 1e-06)
        pre = lax.dot_general(in_ref[...], x, dims, preferred_element_type=jnp.float32) * scale
        gate_pre, up_pre = pre[:units], pre[units:]
        back = lax.dot_general(down_ref[...], tangent[:, lanes], dims, preferred_element_type=jnp.float32)
        root = 0.7978845608028654
        square = gate_pre * gate_pre
        bent = jnp.tanh(root * gate_pre * (1.0 + 0.044715 * square))
        half = 0.5 * (1.0 + bent)
        activated = gate_pre * half
        slope = half + 0.5 * gate_pre * (1.0 - bent * bent) * root * (1.0 + 3 * 0.044715 * square)
        inner[:, lanes] = (activated * up_pre).astype(jnp.bfloat16)
        back_scaled = back * scale
        d_in[:units, lanes] = (back_scaled * up_pre * slope).astype(jnp.bfloat16)
        d_in[units:, lanes] = (back_scaled * activated).astype(jnp.bfloat16)

    wide = SHARE

    @pl.loop(0, count // wide)
    def _(tile):
        forward(pl.ds(pl.multiple_of(tile * wide, wide), wide))

    spans = [(start, min(CHUNK, count - start)) for start in range(0, count, CHUNK)]

    def accumulated(left, right, rows):
        total = comp = None
        for start, size in spans:
            term = lax.dot_general(
                left[:, start : start + size],
                right[rows, start : start + size],
                (((1,), (1,)), ((), ())),
                preferred_element_type=jnp.float32,
            )
            if total is None:
                total, comp = term, jnp.zeros_like(term)
                continue
            adjusted = term - comp
            running = total + adjusted
            comp = (running - total) - adjusted
            total = running
        return total

    @pl.loop(0, D // wide)
    def _(tile):
        rows = pl.ds(pl.multiple_of(tile * wide, wide), wide)
        first = accumulated(d_in, states, rows) * gain_ref[0:1, rows]
        out_ref[tile, 0] = first[:units].astype(jnp.bfloat16)
        out_ref[tile, 1] = first[units:].astype(jnp.bfloat16)
        out_ref[tile, 2] = accumulated(inner, tangent, rows).astype(jnp.bfloat16)


def gradients(pieces, place, gain, wi_gate, wi_up, wo_weight, count):
    arrays = [array for array, *_ in pieces]
    plan = [where for _, *where in pieces]
    units = wi_gate.shape[0]
    w_in = (jnp.concatenate([wi_gate, wi_up]).astype(jnp.float32) * gain).astype(jnp.bfloat16)
    in_vmem = pl.BlockSpec(memory_space=pltpu.VMEM)
    return pl.pallas_call(
        functools.partial(gradients_kernel, plan, count),
        out_shape=jax.ShapeDtypeStruct((D // SHARE, 3, units, SHARE), jnp.bfloat16),
        in_specs=[pl.BlockSpec(memory_space=pltpu.SMEM)]
        + [in_vmem] * 3
        + [pl.BlockSpec(memory_space=pl.ANY)] * len(arrays),
        out_specs=in_vmem,
        scratch_shapes=[
            pltpu.VMEM((D, count), jnp.bfloat16),
            pltpu.VMEM((D, count), jnp.bfloat16),
            pltpu.VMEM((2 * units, count), jnp.bfloat16),
            pltpu.VMEM((units, count), jnp.bfloat16),
            pltpu.SemaphoreType.DMA((2,)),
        ],
        compiler_params=pltpu.CompilerParams(vmem_limit_bytes=60_000_000),
        cost_estimate=pl.CostEstimate(
            flops=12 * units * D * count, bytes_accessed=8 * D * count, transcendentals=units * count
        ),
        name="gradients",
    )(place, gain, w_in, wo_weight, *arrays)


def summed_over_groups(parts, denominator):
    place_x, place_core = lax.axis_index("x"), lax.axis_index("core")
    half = SHARE // 2
    by_core = parts.reshape(2, NX, *parts.shape[1:])
    given = shifted(lax.dynamic_index_in_dim(by_core, 1 - place_core, 0, False), "core", 1)
    pair = lax.dynamic_index_in_dim(by_core, place_core, 0, False).astype(jnp.float32) + given.astype(jnp.float32)

    def due(step):
        return lax.dynamic_index_in_dim(pair, (place_x + step) % NX, 0, False)

    far = due(2).astype(jnp.bfloat16)
    far_ahead = shifted(far[..., :half], "x", 1).astype(jnp.float32)
    far_behind = shifted(far[..., half:], "x", -1).astype(jnp.float32)
    ahead, behind = due(1), due(-1)
    ahead = jnp.concatenate([ahead[..., :half] + far_ahead, ahead[..., half:]], axis=-1)
    behind = jnp.concatenate([behind[..., :half], behind[..., half:] + far_behind], axis=-1)
    from_behind = shifted(ahead.astype(jnp.bfloat16), "x", 1)
    from_ahead = shifted(behind.astype(jnp.bfloat16), "x", -1)
    total = due(0) + from_behind.astype(jnp.float32) + from_ahead.astype(jnp.float32)
    share = (total / denominator).astype(jnp.bfloat16)
    back_1 = shifted(share, "x", 1)
    back_3 = shifted(share, "x", -1)
    back_2 = jnp.concatenate(
        [shifted(back_1[..., :half], "x", 1), shifted(back_3[..., half:], "x", -1)],
        axis=-1,
    )
    own = jnp.stack([share, back_1, back_2, back_3])
    other = shifted(own, "core", 1)
    low = jnp.where(place_core == 0, own, other)
    high = jnp.where(place_core == 0, other, own)
    columns = [
        lax.dynamic_index_in_dim(side, (place_x + NX - x) % NX, 0, False) for side in (low, high) for x in range(NX)
    ]
    return jnp.concatenate(columns, axis=-1).astype(jnp.float32)


def on_device(hidden, gain, cotangent, blocks, loss_mask, wi_gate, wi_up, wo_weight):
    row_count = hidden.shape[2]
    count = hidden.shape[1] * row_count
    feats = hidden.shape[3]
    position = lax.iota(jnp.int32, row_count)
    offset = position % TLEN
    sequence = position // TLEN
    picker = (sequence[None, :] == lax.iota(jnp.int32, blocks.shape[2])[:, None]).astype(jnp.int32)
    limit_pos = jnp.sum(blocks[0][:, :, None] * picker[None, :, :], axis=1) * BLOCK
    weight = (offset[None, :] < limit_pos).astype(jnp.int32) * loss_mask[0]
    tangent = cotangent[0] * weight[:, :, None].astype(jnp.bfloat16)
    own = jnp.stack([jnp.moveaxis(a, 2, 0).reshape(feats, count) for a in (hidden[0], tangent)])
    pieces = gathered(own, 128 * round(count * 0.375 / 128))
    whole_gain = sent_to_all(gain, MP).reshape(1, -1)
    token_total = sent_to_all(jnp.sum(weight), DP).sum(axis=0)
    denominator = jnp.maximum(token_total, 1).astype(jnp.float32)
    place = jnp.stack([lax.axis_index("y"), lax.axis_index("z")]).astype(jnp.int32)
    parts = gradients(pieces, place, whole_gain, wi_gate, wi_up, wo_weight, count)
    return summed_over_groups(parts, denominator)


def solution(mesh):
    torus = Mesh(mesh.devices.reshape(4, 2, NY, NZ), ("x", "core", "y", "z"))

    return jax.shard_map(
        on_device,
        mesh=torus,
        in_specs=(
            P(DP, None, None, MP),
            P(MP),
            P(DP, None, None, MP),
            P(DP, None, None),
            P(DP, None, None),
            P(MP, None),
            P(MP, None),
            P(MP, None),
        ),
        out_specs=P(None, MP, None),
        check_vma=False,
    )
```

```python
import functools

import jax
import jax.numpy as jnp
from jax import lax
from jax.experimental import pallas as pl
from jax.experimental.pallas import tpu as pltpu
from jax.sharding import Mesh
from jax.sharding import PartitionSpec as P


D = 2048
BLOCK = 128
TLEN = 256
DP = ("x", "core")
MP = ("y", "z")
NY = 4
NZ = 8
CHUNK = 512
SHARE = 256
NX = 4
LENGTHS = (512, 1024, 512)
GROUPS_Z = ((7, 3), (2, 5))


def sent_to_all(x, axis):
    devices = lax.axis_size(axis)
    return lax.all_to_all(jnp.broadcast_to(x[None], (devices, *x.shape)), axis, 0, 0, tiled=True)


def shifted(x, axis, step):
    size = lax.axis_size(axis)
    return lax.ppermute(x, axis, [(i, (i + step) % size) for i in range(size)])


def ring(own, axis, tensor_dim):
    size = lax.axis_size(axis)
    ahead, behind = own, own
    blocks = {0: own}
    for step in range(1, size // 2):
        ahead = shifted(ahead, axis, 1)
        behind = shifted(behind, axis, -1)
        blocks[step], blocks[size - step] = ahead, behind
    first = lax.index_in_dim(ahead, 0, tensor_dim, keepdims=False)
    second = lax.index_in_dim(behind, 1, tensor_dim, keepdims=False)
    last = size // 2
    blocks[last] = (shifted(first, axis, 1), shifted(second, axis, -1))
    return blocks


def joined(blocks, order):
    return jnp.stack([jnp.stack(b) if isinstance(b, tuple) else b for b in (blocks[k] for k in order)])


def gathered(part_a, part_b):
    first = part_a.shape[-1]
    pieces = []

    def add(got, *where):
        if isinstance(got, tuple):
            for tensor, array in enumerate(got):
                pieces.append((array, (tensor,), *where))
        else:
            pieces.append((got, (0, 1), *where))

    rows_b = ring(part_b, "z", 0)
    column_a = ring(part_a, "y", 0)
    joined_a = joined(column_a, range(NY))
    for back_z, got in ring(joined_a, "z", 1).items():
        add(got, 0, back_z, "y", 0)
    for least, many in GROUPS_Z:
        group = joined(rows_b, [(least + k) % NZ for k in range(many)])
        for back_y, got in ring(group, "y", 1).items():
            add(got, back_y, least, "z", first)
    return pieces


def turned(rows, out_ref):
    square = jnp.concatenate([rows, jnp.zeros((128 - rows.shape[0], 128), rows.dtype)]).T
    for k in range(rows.shape[0]):
        out_ref[k * 128 : k * 128 + 128, :] = square[:, k : k + 1]


def counted_kernel(micro_count, blocks_ref, mask_ref, hidden_ref, cotangent_ref, *refs):
    outs, total_ref, place_ref = refs[:-2], refs[-2], refs[-1]
    per_micro = hidden_ref.shape[2] // BLOCK
    per_sequence = TLEN // BLOCK
    rows = micro_count * per_micro
    weight = []
    for row in range(rows):
        micro, block = row // per_micro, row % per_micro
        used = blocks_ref[micro, block // per_sequence] > block % per_sequence
        weight.append(mask_ref[row : row + 1, :] * used.astype(jnp.int32))
    weight = jnp.concatenate(weight).astype(jnp.float32)
    narrow = weight.astype(jnp.bfloat16)
    dims = (((1,), (0,)), ((), ()))

    def triangle(size, strict):
        one, two = (lax.broadcasted_iota(jnp.int32, (size, size), k) for k in (0, 1))
        return (one > two if strict else one <= two).astype(jnp.float32).astype(jnp.bfloat16)

    within = lax.dot_general(narrow, triangle(128, False), dims, preferred_element_type=jnp.float32)
    before = lax.dot_general(triangle(rows, True), narrow, dims, preferred_element_type=jnp.float32)
    rank = within + jnp.sum(before, axis=1, keepdims=True) - 1.0
    turned(jnp.where(weight > 0, rank, -1.0), place_ref)
    total_ref[...] = jnp.broadcast_to(jnp.sum(weight), total_ref.shape)
    wide = 256
    into = [(out, start) for out in outs for start in range(0, out.shape[2], wide)]
    for tile, (out, start) in enumerate(into):
        slots = (lax.broadcasted_iota(jnp.int32, (1, wide), 1) + tile * wide).astype(jnp.float32)
        sums = jnp.zeros((2 * hidden_ref.shape[1], wide), jnp.float32)
        for row in range(tile * wide // BLOCK, rows):
            micro, lanes = row // per_micro, pl.ds(row % per_micro * BLOCK, BLOCK)
            values = jnp.concatenate([hidden_ref[micro, :, lanes], cotangent_ref[micro, :, lanes]])
            chosen = place_ref[row * BLOCK : row * BLOCK + BLOCK, :] == slots
            chosen = chosen.astype(jnp.float32).astype(jnp.bfloat16)
            sums += lax.dot_general(values, chosen, dims, preferred_element_type=jnp.float32)
        feats = hidden_ref.shape[1]
        out[0, :, start : start + wide] = sums[:feats].astype(jnp.bfloat16)
        out[1, :, start : start + wide] = sums[feats:].astype(jnp.bfloat16)


def counted_first(hidden, cotangent, blocks, loss_mask, lengths):
    micro_count, row_count, feats = hidden.shape
    in_vmem = pl.BlockSpec(memory_space=pltpu.VMEM)
    count = micro_count * row_count
    *parts, total = pl.pallas_call(
        functools.partial(counted_kernel, micro_count),
        out_shape=[jax.ShapeDtypeStruct((2, feats, length), jnp.bfloat16) for length in lengths]
        + [jax.ShapeDtypeStruct((8, 128), jnp.float32)],
        in_specs=[pl.BlockSpec(memory_space=pltpu.SMEM)] + [in_vmem] * 3,
        out_specs=[in_vmem] * (len(lengths) + 1),
        scratch_shapes=[pltpu.VMEM((count, 1), jnp.float32)],
        cost_estimate=pl.CostEstimate(flops=2 * feats * count * count, bytes_accessed=8 * feats * count, transcendentals=0),
        name="counted_first",
    )(
        blocks,
        loss_mask.reshape(count // BLOCK, BLOCK),
        jnp.swapaxes(hidden, 1, 2),
        jnp.swapaxes(cotangent, 1, 2),
    )
    return parts, total[0, 0].astype(jnp.int32)


def gradients_kernel(plan, count, place_ref, gain_ref, in_ref, down_ref, *refs):
    pieces, out_ref = refs[: len(plan)], refs[len(plan)]
    states, tangent, d_in, inner, gain_column, sems = refs[len(plan) + 1 :]
    place_y, place_z = place_ref[0], place_ref[1]
    feats, units = D // (NY * NZ), down_ref.shape[0]

    def rows_of(back_y, back_z):
        row_y = lax.rem(place_y + NY - back_y, NY)
        row_z = lax.rem(place_z + NZ - back_z, NZ)
        return pl.ds(pl.multiple_of((row_y * NZ + row_z) * feats, feats), feats)

    copies = ([], [])
    for tensor, whole in enumerate((states, tangent)):
        for ref, (tensors, back_y, back_z, along, base) in zip(pieces, plan):
            if tensor not in tensors:
                continue
            for k in range(ref.shape[0]):
                if along == "all":
                    rows = pl.ds(k * feats, feats)
                else:
                    rows = rows_of(k, back_z) if along == "y" else rows_of(back_y, (back_z + k) % NZ)
                copies[tensor].append(
                    pltpu.make_async_copy(
                        ref.at[k, tensor] if len(tensors) > 1 else ref.at[k],
                        whole.at[rows, pl.ds(base, ref.shape[-1])],
                        sems.at[tensor],
                    )
                )
                copies[tensor][-1].start()
    turned(gain_ref[...], gain_column)
    for copy in copies[0]:
        copy.wait()
    wide = SHARE
    height = 256

    @pl.loop(0, count // wide)
    def _(tile):
        lanes = pl.ds(pl.multiple_of(tile * wide, wide), wide)
        squares = jnp.zeros((8, wide), jnp.float32)
        for top in range(0, D, height):
            x = states[top : top + height, lanes].astype(jnp.float32)
            squares += (x * x).reshape(height // 8, 8, wide).sum(axis=0)
        scale = lax.rsqrt(jnp.sum(squares, axis=0, keepdims=True) / D + 1e-06)
        for top in range(0, D, height):
            x = states[top : top + height, lanes].astype(jnp.float32)
            gain = gain_column[top : top + height, :]
            states[top : top + height, lanes] = (x * scale * gain).astype(jnp.bfloat16)

    for copy in copies[1]:
        copy.wait()

    def forward(lanes):
        dims = (((1,), (0,)), ((), ()))
        pre = lax.dot_general(in_ref[...], states[:, lanes], dims, preferred_element_type=jnp.float32)
        gate_pre, up_pre = pre[:units], pre[units:]
        back = lax.dot_general(down_ref[...], tangent[:, lanes], dims, preferred_element_type=jnp.float32)
        root = 0.7978845608028654
        square = gate_pre * gate_pre
        bent = jnp.tanh(root * gate_pre * (1.0 + 0.044715 * square))
        half = 0.5 * (1.0 + bent)
        activated = gate_pre * half
        slope = half + 0.5 * gate_pre * (1.0 - bent * bent) * root * (1.0 + 3 * 0.044715 * square)
        inner[:, lanes] = (activated * up_pre).astype(jnp.bfloat16)
        d_in[:units, lanes] = (back * up_pre * slope).astype(jnp.bfloat16)
        d_in[units:, lanes] = (back * activated).astype(jnp.bfloat16)

    @pl.loop(0, count // wide)
    def _(tile):
        forward(pl.ds(pl.multiple_of(tile * wide, wide), wide))

    spans = [(start, min(CHUNK, count - start)) for start in range(0, count, CHUNK)]

    def accumulated(left, right, rows):
        total = comp = None
        for start, size in spans:
            term = lax.dot_general(
                left[:, start : start + size],
                right[rows, start : start + size],
                (((1,), (1,)), ((), ())),
                preferred_element_type=jnp.float32,
            )
            if total is None:
                total, comp = term, jnp.zeros_like(term)
                continue
            adjusted = term - comp
            running = total + adjusted
            comp = (running - total) - adjusted
            total = running
        return total

    @pl.loop(0, D // wide)
    def _(tile):
        rows = pl.ds(pl.multiple_of(tile * wide, wide), wide)
        first = accumulated(d_in, states, rows)
        out_ref[tile, 0] = first[:units].astype(jnp.bfloat16)
        out_ref[tile, 1] = first[units:].astype(jnp.bfloat16)
        out_ref[tile, 2] = accumulated(inner, tangent, rows).astype(jnp.bfloat16)


def gradients(pieces, place, gain, wi_gate, wi_up, wo_weight, count):
    arrays = [array for array, *_ in pieces]
    plan = [where for _, *where in pieces]
    units = wi_gate.shape[0]
    w_in = jnp.concatenate([wi_gate, wi_up])
    in_vmem = pl.BlockSpec(memory_space=pltpu.VMEM)
    return pl.pallas_call(
        functools.partial(gradients_kernel, plan, count),
        out_shape=jax.ShapeDtypeStruct((D // SHARE, 3, units, SHARE), jnp.bfloat16),
        in_specs=[pl.BlockSpec(memory_space=pltpu.SMEM)]
        + [in_vmem] * 3
        + [pl.BlockSpec(memory_space=pl.ANY)] * len(arrays),
        out_specs=in_vmem,
        scratch_shapes=[
            pltpu.VMEM((D, count), jnp.bfloat16),
            pltpu.VMEM((D, count), jnp.bfloat16),
            pltpu.VMEM((2 * units, count), jnp.bfloat16),
            pltpu.VMEM((units, count), jnp.bfloat16),
            pltpu.VMEM((D, 1), jnp.float32),
            pltpu.SemaphoreType.DMA((2,)),
        ],
        compiler_params=pltpu.CompilerParams(vmem_limit_bytes=60_000_000),
        cost_estimate=pl.CostEstimate(
            flops=12 * units * D * count, bytes_accessed=8 * D * count, transcendentals=units * count
        ),
        name="gradients",
    )(place, gain, w_in, wo_weight, *arrays)


def summed_over_groups(parts, denominator):
    place_x, place_core = lax.axis_index("x"), lax.axis_index("core")
    half = SHARE // 2
    by_core = parts.reshape(2, NX, *parts.shape[1:])
    given = shifted(lax.dynamic_index_in_dim(by_core, 1 - place_core, 0, False), "core", 1)
    pair = lax.dynamic_index_in_dim(by_core, place_core, 0, False).astype(jnp.float32) + given.astype(jnp.float32)

    def due(step):
        return lax.dynamic_index_in_dim(pair, (place_x + step) % NX, 0, False)

    far = due(2).astype(jnp.bfloat16)
    far_ahead = shifted(far[..., :half], "x", 1).astype(jnp.float32)
    far_behind = shifted(far[..., half:], "x", -1).astype(jnp.float32)
    ahead, behind = due(1), due(-1)
    ahead = jnp.concatenate([ahead[..., :half] + far_ahead, ahead[..., half:]], axis=-1)
    behind = jnp.concatenate([behind[..., :half], behind[..., half:] + far_behind], axis=-1)
    from_behind = shifted(ahead.astype(jnp.bfloat16), "x", 1)
    from_ahead = shifted(behind.astype(jnp.bfloat16), "x", -1)
    total = due(0) + from_behind.astype(jnp.float32) + from_ahead.astype(jnp.float32)
    share = (total / denominator).astype(jnp.bfloat16)
    back_1 = shifted(share, "x", 1)
    back_3 = shifted(share, "x", -1)
    back_2 = jnp.concatenate(
        [shifted(back_1[..., :half], "x", 1), shifted(back_3[..., half:], "x", -1)],
        axis=-1,
    )
    own = jnp.stack([share, back_1, back_2, back_3])
    other = shifted(own, "core", 1)
    low = jnp.where(place_core == 0, own, other)
    high = jnp.where(place_core == 0, other, own)
    columns = [
        lax.dynamic_index_in_dim(side, (place_x + NX - x) % NX, 0, False) for side in (low, high) for x in range(NX)
    ]
    return jnp.concatenate(columns, axis=-1).astype(jnp.float32)


def on_device(hidden, gain, cotangent, blocks, loss_mask, wi_gate, wi_up, wo_weight):
    (part_a, part_b, rest), own_total = counted_first(hidden[0], cotangent[0], blocks[0], loss_mask[0], LENGTHS)
    pieces = gathered(part_a, part_b)
    whole_gain = sent_to_all(gain, MP).reshape(-1, 128)
    totals = sent_to_all(own_total, DP)
    denominator = jnp.maximum(totals.sum(), 1).astype(jnp.float32)
    place = jnp.stack([lax.axis_index("y"), lax.axis_index("z")]).astype(jnp.int32)
    weights = (wi_gate, wi_up, wo_weight)
    parts = gradients(pieces, place, whole_gain, *weights, sum(LENGTHS[:2]))

    def with_rest(parts):
        got = sent_to_all(rest, MP)
        more = gradients([(got, (0, 1), 0, 0, "all", 0)], place, whole_gain, *weights, LENGTHS[2])
        return (parts.astype(jnp.float32) + more.astype(jnp.float32)).astype(jnp.bfloat16)

    parts = lax.cond(jnp.max(totals) > sum(LENGTHS[:2]), with_rest, lambda parts: parts, parts)
    return summed_over_groups(parts, denominator)


def solution(mesh):
    torus = Mesh(mesh.devices.reshape(4, 2, NY, NZ), ("x", "core", "y", "z"))

    return jax.shard_map(
        on_device,
        mesh=torus,
        in_specs=(
            P(DP, None, None, MP),
            P(MP),
            P(DP, None, None, MP),
            P(DP, None, None),
            P(DP, None, None),
            P(MP, None),
            P(MP, None),
            P(MP, None),
        ),
        out_specs=P(None, MP, None),
        check_vma=False,
    )
```

```python
import functools

import jax
import jax.numpy as jnp
from jax import lax
from jax.experimental import pallas as pl
from jax.experimental.pallas import tpu as pltpu
from jax.sharding import Mesh
from jax.sharding import PartitionSpec as P


D = 2048
BLOCK = 128
TLEN = 256
DP = ("x", "core")
MP = ("y", "z")
NY = 4
NZ = 8
CHUNK = 512
SHARE = 256
NX = 4
LENGTHS = (512, 1024, 768)
ALWAYS = LENGTHS[0] + LENGTHS[1]
ADDENDS = 3
GROUPS_Z = ((7, 3), (2, 5))


def sent_to_all(x, axis):
    devices = lax.axis_size(axis)
    return lax.all_to_all(jnp.broadcast_to(x[None], (devices, *x.shape)), axis, 0, 0, tiled=True)


def shifted(x, axis, step):
    size = lax.axis_size(axis)
    return lax.ppermute(x, axis, [(i, (i + step) % size) for i in range(size)])


def ring(own, axis, cut):
    size = lax.axis_size(axis)
    ahead, behind = own, own
    blocks = {0: own}
    for step in range(1, size // 2):
        ahead = shifted(ahead, axis, 1)
        behind = shifted(behind, axis, -1)
        blocks[step], blocks[size - step] = ahead, behind
    last = size // 2
    blocks[last] = (shifted(ahead[:cut], axis, 1), shifted(behind[cut:], axis, -1))
    return blocks


def joined(blocks, order):
    return jnp.stack([jnp.concatenate(b) if isinstance(b, tuple) else b for b in (blocks[k] for k in order)])


def gathered(part_a, part_b):
    first = part_a.shape[-1]
    pieces = []
    rows_b = ring(part_b, "z", 1)
    joined_a = joined(ring(part_a, "y", 1), range(NY))
    for back_z, got in ring(joined_a, "z", NY // 2).items():
        if isinstance(got, tuple):
            pieces.append((got[0], 0, back_z, "y", 0))
            pieces.append((got[1], NY // 2, back_z, "y", 0))
        else:
            pieces.append((got, 0, back_z, "y", 0))
    for (least, many), cut in zip(GROUPS_Z, (1, 3)):
        group = joined(rows_b, [(least + k) % NZ for k in range(many)])
        for back_y, got in ring(group, "y", cut).items():
            if isinstance(got, tuple):
                pieces.append((got[0], back_y, least, "z", first))
                pieces.append((got[1], back_y, least + cut, "z", first))
            else:
                pieces.append((got, back_y, least, "z", first))
    return pieces


def turned(rows, out_ref):
    square = jnp.concatenate([rows, jnp.zeros((128 - rows.shape[0], 128), rows.dtype)]).T
    for k in range(rows.shape[0]):
        out_ref[k * 128 : k * 128 + 128, :] = square[:, k : k + 1]


def counted_kernel(blocks_ref, mask_ref, gain_ref, hidden_ref, cotangent_ref, *refs):
    outs, total_ref, place_ref = refs[:-2], refs[-2], refs[-1]
    micro_count, feats, row_count = hidden_ref.shape
    per_micro, per_sequence = row_count // BLOCK, TLEN // BLOCK
    rows = micro_count * per_micro
    weight = []
    for row in range(rows):
        micro, block = row // per_micro, row % per_micro
        sequence = block // per_sequence
        used = blocks_ref[sequence : sequence + 1, micro : micro + 1] > block % per_sequence
        mask = mask_ref[micro : micro + 1, block * BLOCK : block * BLOCK + BLOCK]
        weight.append(jnp.where(used, mask, 0))
    weight = jnp.concatenate(weight).astype(jnp.float32)
    narrow = weight.astype(jnp.bfloat16)
    dims = (((1,), (0,)), ((), ()))

    def triangle(size, strict):
        one, two = (lax.broadcasted_iota(jnp.int32, (size, size), k) for k in (0, 1))
        return (one > two if strict else one <= two).astype(jnp.float32).astype(jnp.bfloat16)

    within = lax.dot_general(narrow, triangle(BLOCK, False), dims, preferred_element_type=jnp.float32)
    before = lax.dot_general(triangle(rows, True), narrow, dims, preferred_element_type=jnp.float32)
    rank = within + jnp.sum(before, axis=1, keepdims=True) - 1.0
    slot = jnp.where(rank < ALWAYS - ADDENDS, rank, rank + ADDENDS)
    turned(jnp.where(weight > 0, slot, -1.0), place_ref)
    total_ref[...] = jnp.broadcast_to(jnp.sum(weight), total_ref.shape)
    one, two = (lax.broadcasted_iota(jnp.int32, (feats, feats), k) for k in (0, 1))
    left = jnp.sum(jnp.where(one == two, gain_ref[...], 0.0), axis=1, keepdims=True)
    addends = []
    for _ in range(ADDENDS):
        addends.append(left.astype(jnp.bfloat16).astype(jnp.float32))
        left = left - addends[-1]
    wide = SHARE
    into = [(out, start) for out in outs for start in range(0, out.shape[2], wide)]
    for tile, (out, start) in enumerate(into):
        lane = lax.broadcasted_iota(jnp.int32, (1, wide), 1)
        slots = (lane + tile * wide).astype(jnp.float32)
        sums = jnp.zeros((2 * feats, wide), jnp.float32)
        for row in range(max(tile * wide - ADDENDS, 0) // BLOCK, rows):
            micro, lanes = row // per_micro, pl.ds(row % per_micro * BLOCK, BLOCK)
            values = jnp.concatenate([hidden_ref[micro, :, lanes], cotangent_ref[micro, :, lanes]])
            chosen = place_ref[row * BLOCK : row * BLOCK + BLOCK, :] == slots
            chosen = chosen.astype(jnp.float32).astype(jnp.bfloat16)
            sums += lax.dot_general(values, chosen, dims, preferred_element_type=jnp.float32)
        states = sums[:feats]
        if (tile + 1) * wide in (ALWAYS, sum(LENGTHS)):
            for k, addend in enumerate(addends):
                states = jnp.where(lane == wide - ADDENDS + k, addend, states)
        out[0, :, start : start + wide] = states.astype(jnp.bfloat16)
        out[1, :, start : start + wide] = sums[feats:].astype(jnp.bfloat16)


def counted_first(hidden, cotangent, blocks, loss_mask, gain):
    micro_count, row_count, feats = hidden.shape
    in_vmem = pl.BlockSpec(memory_space=pltpu.VMEM)
    count = micro_count * row_count
    *parts, total = pl.pallas_call(
        counted_kernel,
        out_shape=[jax.ShapeDtypeStruct((2, feats, length), jnp.bfloat16) for length in LENGTHS]
        + [jax.ShapeDtypeStruct((8, 128), jnp.float32)],
        in_specs=[in_vmem] * 5,
        out_specs=[in_vmem] * (len(LENGTHS) + 1),
        scratch_shapes=[pltpu.VMEM((count, 1), jnp.float32)],
        cost_estimate=pl.CostEstimate(flops=2 * feats * count * count, bytes_accessed=8 * feats * count, transcendentals=0),
        name="counted_first",
    )(
        blocks.T,
        loss_mask,
        gain.reshape(1, -1),
        jnp.swapaxes(hidden, 1, 2),
        jnp.swapaxes(cotangent, 1, 2),
    )
    return parts, total[0, 0].astype(jnp.int32)


def gradients_kernel(plan, count, gate_ref, up_ref, down_ref, *refs):
    pieces, out_ref = refs[: len(plan)], refs[len(plan)]
    states, tangent, d_in, inner, in_ref, gain_column, sems = refs[len(plan) + 1 :]
    place_y, place_z = lax.axis_index("y"), lax.axis_index("z")
    feats, units = D // (NY * NZ), down_ref.shape[0]

    def rows_of(back_y, back_z):
        row_y = lax.rem(place_y + 2 * NY - back_y, NY)
        row_z = lax.rem(place_z + 2 * NZ - back_z, NZ)
        return pl.ds(pl.multiple_of((row_y * NZ + row_z) * feats, feats), feats)

    copies = ([], [])
    for tensor, whole in enumerate((states, tangent)):
        for ref, (back_y, back_z, along, base) in zip(pieces, plan):
            for k in range(ref.shape[0]):
                if along == "all":
                    rows = pl.ds(k * feats, feats)
                else:
                    rows = rows_of(back_y + k, back_z) if along == "y" else rows_of(back_y, back_z + k)
                into = whole.at[rows, pl.ds(base, ref.shape[-1])]
                copies[tensor].append(pltpu.make_async_copy(ref.at[k, tensor], into, sems.at[tensor]))
                copies[tensor][-1].start()
    in_ref[:units, :] = gate_ref[...]
    in_ref[units:, :] = up_ref[...]
    for copy in copies[0]:
        copy.wait()
    wide = SHARE
    height = 256
    addends = states[:, count - 128 : count].astype(jnp.float32)
    lane = lax.broadcasted_iota(jnp.int32, (1, 128), 1)
    gain_column[...] = jnp.sum(jnp.where(lane >= 128 - ADDENDS, addends, 0.0), axis=1, keepdims=True)

    @pl.loop(0, count // wide)
    def _(tile):
        lanes = pl.ds(pl.multiple_of(tile * wide, wide), wide)
        squares = jnp.zeros((8, wide), jnp.float32)
        for top in range(0, D, height):
            x = states[top : top + height, lanes].astype(jnp.float32)
            squares += (x * x).reshape(height // 8, 8, wide).sum(axis=0)
        scale = lax.rsqrt(jnp.sum(squares, axis=0, keepdims=True) / D + 1e-06)
        for top in range(0, D, height):
            x = states[top : top + height, lanes].astype(jnp.float32)
            gain = gain_column[top : top + height, :]
            states[top : top + height, lanes] = (x * scale * gain).astype(jnp.bfloat16)

    for copy in copies[1]:
        copy.wait()

    def forward(lanes):
        dims = (((1,), (0,)), ((), ()))
        pre = lax.dot_general(in_ref[...], states[:, lanes], dims, preferred_element_type=jnp.float32)
        gate_pre, up_pre = pre[:units], pre[units:]
        back = lax.dot_general(down_ref[...], tangent[:, lanes], dims, preferred_element_type=jnp.float32)
        root = 0.7978845608028654
        square = gate_pre * gate_pre
        bent = jnp.tanh(root * gate_pre * (1.0 + 0.044715 * square))
        half = 0.5 * (1.0 + bent)
        activated = gate_pre * half
        slope = half + 0.5 * gate_pre * (1.0 - bent * bent) * root * (1.0 + 3 * 0.044715 * square)
        inner[:, lanes] = (activated * up_pre).astype(jnp.bfloat16)
        d_in[:units, lanes] = (back * up_pre * slope).astype(jnp.bfloat16)
        d_in[units:, lanes] = (back * activated).astype(jnp.bfloat16)

    @pl.loop(0, count // wide)
    def _(tile):
        forward(pl.ds(pl.multiple_of(tile * wide, wide), wide))

    spans = [(start, min(CHUNK, count - start)) for start in range(0, count, CHUNK)]

    def accumulated(left, right, rows):
        total = comp = None
        for start, size in spans:
            term = lax.dot_general(
                left[:, start : start + size],
                right[rows, start : start + size],
                (((1,), (1,)), ((), ())),
                preferred_element_type=jnp.float32,
            )
            if total is None:
                total, comp = term, jnp.zeros_like(term)
                continue
            adjusted = term - comp
            running = total + adjusted
            comp = (running - total) - adjusted
            total = running
        return total

    @pl.loop(0, D // wide)
    def _(tile):
        rows = pl.ds(pl.multiple_of(tile * wide, wide), wide)
        first = accumulated(d_in, states, rows)
        out_ref[tile, 0] = first[:units].astype(jnp.bfloat16)
        out_ref[tile, 1] = first[units:].astype(jnp.bfloat16)
        out_ref[tile, 2] = accumulated(inner, tangent, rows).astype(jnp.bfloat16)


def gradients(pieces, wi_gate, wi_up, wo_weight, count):
    arrays = [array for array, *_ in pieces]
    plan = [where for _, *where in pieces]
    units = wi_gate.shape[0]
    in_vmem = pl.BlockSpec(memory_space=pltpu.VMEM)
    return pl.pallas_call(
        functools.partial(gradients_kernel, plan, count),
        out_shape=jax.ShapeDtypeStruct((D // SHARE, 3, units, SHARE), jnp.bfloat16),
        in_specs=[in_vmem] * 3 + [pl.BlockSpec(memory_space=pl.ANY)] * len(arrays),
        out_specs=in_vmem,
        scratch_shapes=[
            pltpu.VMEM((D, count), jnp.bfloat16),
            pltpu.VMEM((D, count), jnp.bfloat16),
            pltpu.VMEM((2 * units, count), jnp.bfloat16),
            pltpu.VMEM((units, count), jnp.bfloat16),
            pltpu.VMEM((2 * units, D), jnp.bfloat16),
            pltpu.VMEM((D, 1), jnp.float32),
            pltpu.SemaphoreType.DMA((2,)),
        ],
        compiler_params=pltpu.CompilerParams(vmem_limit_bytes=60_000_000),
        cost_estimate=pl.CostEstimate(
            flops=12 * units * D * count, bytes_accessed=8 * D * count, transcendentals=units * count
        ),
        name="gradients",
    )(wi_gate, wi_up, wo_weight, *arrays)


def summed_over_groups(parts, denominator):
    place_x, place_core = lax.axis_index("x"), lax.axis_index("core")
    half = SHARE // 2
    by_core = parts.reshape(2, NX, *parts.shape[1:])
    given = shifted(lax.dynamic_index_in_dim(by_core, 1 - place_core, 0, False), "core", 1)
    pair = lax.dynamic_index_in_dim(by_core, place_core, 0, False).astype(jnp.float32) + given.astype(jnp.float32)

    def due(step):
        return lax.dynamic_index_in_dim(pair, (place_x + step) % NX, 0, False)

    far = due(2).astype(jnp.bfloat16)
    far_ahead = shifted(far[..., :half], "x", 1).astype(jnp.float32)
    far_behind = shifted(far[..., half:], "x", -1).astype(jnp.float32)
    ahead, behind = due(1), due(-1)
    ahead = jnp.concatenate([ahead[..., :half] + far_ahead, ahead[..., half:]], axis=-1)
    behind = jnp.concatenate([behind[..., :half], behind[..., half:] + far_behind], axis=-1)
    from_behind = shifted(ahead.astype(jnp.bfloat16), "x", 1)
    from_ahead = shifted(behind.astype(jnp.bfloat16), "x", -1)
    total = due(0) + from_behind.astype(jnp.float32) + from_ahead.astype(jnp.float32)
    share = (total / denominator).astype(jnp.bfloat16)
    back_1 = shifted(share, "x", 1)
    back_3 = shifted(share, "x", -1)
    back_2 = jnp.concatenate(
        [shifted(back_1[..., :half], "x", 1), shifted(back_3[..., half:], "x", -1)],
        axis=-1,
    )
    own = jnp.stack([share, back_1, back_2, back_3])
    other = shifted(own, "core", 1)
    low = jnp.where(place_core == 0, own, other)
    high = jnp.where(place_core == 0, other, own)
    columns = [
        lax.dynamic_index_in_dim(side, (place_x + NX - x) % NX, 0, False) for side in (low, high) for x in range(NX)
    ]
    return jnp.concatenate(columns, axis=-1).astype(jnp.float32)


def on_device(hidden, gain, cotangent, blocks, loss_mask, wi_gate, wi_up, wo_weight):
    (part_a, part_b, rest), own_total = counted_first(hidden[0], cotangent[0], blocks[0], loss_mask[0], gain)
    pieces = gathered(part_a, part_b)
    totals = sent_to_all(own_total, DP)
    denominator = jnp.maximum(totals.sum(), 1).astype(jnp.float32)
    weights = (wi_gate, wi_up, wo_weight)
    parts = gradients(pieces, *weights, ALWAYS)

    def with_rest(parts):
        got = sent_to_all(rest, MP)
        more = gradients([(got, 0, 0, "all", 0)], *weights, LENGTHS[2])
        return (parts.astype(jnp.float32) + more.astype(jnp.float32)).astype(jnp.bfloat16)

    parts = lax.cond(jnp.max(totals) > ALWAYS - ADDENDS, with_rest, lambda parts: parts, parts)
    return summed_over_groups(parts, denominator)


def solution(mesh):
    torus = Mesh(mesh.devices.reshape(4, 2, NY, NZ), ("x", "core", "y", "z"))

    return jax.shard_map(
        on_device,
        mesh=torus,
        in_specs=(
            P(DP, None, None, MP),
            P(MP),
            P(DP, None, None, MP),
            P(DP, None, None),
            P(DP, None, None),
            P(MP, None),
            P(MP, None),
            P(MP, None),
        ),
        out_specs=P(None, MP, None),
        check_vma=False,
    )
```

```python
import functools

import jax
import jax.numpy as jnp
from jax import lax
from jax.experimental import pallas as pl
from jax.experimental.pallas import tpu as pltpu
from jax.sharding import Mesh
from jax.sharding import PartitionSpec as P


D = 2048
BLOCK = 128
TLEN = 256
DP = ("x", "core")
MP = ("y", "z")
NY = 4
NZ = 8
CHUNK = 512
SHARE = 256
NX = 4
LENGTHS = (512, 1024, 768)
ALWAYS = LENGTHS[0] + LENGTHS[1]
ADDENDS = 3
GROUPS_Z = ((7, 3), (2, 5))


def sent_to_all(x, axis):
    devices = lax.axis_size(axis)
    return lax.all_to_all(jnp.broadcast_to(x[None], (devices, *x.shape)), axis, 0, 0, tiled=True)


def shifted(x, axis, step):
    size = lax.axis_size(axis)
    return lax.ppermute(x, axis, [(i, (i + step) % size) for i in range(size)])


def ring(own, axis, cut):
    size = lax.axis_size(axis)
    ahead, behind = own, own
    blocks = {0: own}
    for step in range(1, size // 2):
        ahead = shifted(ahead, axis, 1)
        behind = shifted(behind, axis, -1)
        blocks[step], blocks[size - step] = ahead, behind
    last = size // 2
    blocks[last] = (shifted(ahead[:cut], axis, 1), shifted(behind[cut:], axis, -1))
    return blocks


def joined(blocks, order):
    return jnp.stack([jnp.concatenate(b) if isinstance(b, tuple) else b for b in (blocks[k] for k in order)])


def gathered(part_a, part_b):
    first = part_a.shape[-1]
    pieces = []
    rows_b = ring(part_b, "z", 1)
    joined_a = joined(ring(part_a, "y", 1), range(NY))
    for back_z, got in ring(joined_a, "z", NY // 2).items():
        if isinstance(got, tuple):
            pieces.append((got[0], 0, back_z, "y", 0))
            pieces.append((got[1], NY // 2, back_z, "y", 0))
        else:
            pieces.append((got, 0, back_z, "y", 0))
    for (least, many), cut in zip(GROUPS_Z, (1, 3)):
        group = joined(rows_b, [(least + k) % NZ for k in range(many)])
        for back_y, got in ring(group, "y", cut).items():
            if isinstance(got, tuple):
                pieces.append((got[0], back_y, least, "z", first))
                pieces.append((got[1], back_y, least + cut, "z", first))
            else:
                pieces.append((got, back_y, least, "z", first))
    return pieces


def turned(rows, out_ref):
    square = jnp.concatenate([rows, jnp.zeros((128 - rows.shape[0], 128), rows.dtype)]).T
    for k in range(rows.shape[0]):
        out_ref[k * 128 : k * 128 + 128, :] = square[:, k : k + 1]


def counted_kernel(blocks_ref, mask_ref, gain_ref, hidden_ref, cotangent_ref, *refs):
    outs, total_ref, place_ref = refs[:-2], refs[-2], refs[-1]
    micro_count, feats, row_count = hidden_ref.shape
    per_micro, per_sequence = row_count // BLOCK, TLEN // BLOCK
    rows = micro_count * per_micro
    weight = []
    for row in range(rows):
        micro, block = row // per_micro, row % per_micro
        sequence = block // per_sequence
        used = blocks_ref[sequence : sequence + 1, micro : micro + 1] > block % per_sequence
        mask = mask_ref[micro : micro + 1, block * BLOCK : block * BLOCK + BLOCK]
        weight.append(jnp.where(used, mask, 0))
    weight = jnp.concatenate(weight).astype(jnp.float32)
    narrow = weight.astype(jnp.bfloat16)
    dims = (((1,), (0,)), ((), ()))

    def triangle(size, strict):
        one, two = (lax.broadcasted_iota(jnp.int32, (size, size), k) for k in (0, 1))
        return (one > two if strict else one <= two).astype(jnp.float32).astype(jnp.bfloat16)

    within = lax.dot_general(narrow, triangle(BLOCK, False), dims, preferred_element_type=jnp.float32)
    before = lax.dot_general(triangle(rows, True), narrow, dims, preferred_element_type=jnp.float32)
    rank = within + jnp.sum(before, axis=1, keepdims=True) - 1.0
    slot = jnp.where(rank < ALWAYS - ADDENDS, rank, rank + ADDENDS)
    turned(jnp.where(weight > 0, slot, -1.0), place_ref)
    total_ref[...] = jnp.broadcast_to(jnp.sum(weight), total_ref.shape)
    one, two = (lax.broadcasted_iota(jnp.int32, (feats, feats), k) for k in (0, 1))
    left = jnp.sum(jnp.where(one == two, gain_ref[...], 0.0), axis=1, keepdims=True)
    addends = []
    for _ in range(ADDENDS):
        addends.append(left.astype(jnp.bfloat16).astype(jnp.float32))
        left = left - addends[-1]
    wide = SHARE
    into = [(out, start) for out in outs for start in range(0, out.shape[2], wide)]
    for tile, (out, start) in enumerate(into):
        lane = lax.broadcasted_iota(jnp.int32, (1, wide), 1)
        slots = (lane + tile * wide).astype(jnp.float32)
        sums = jnp.zeros((2 * feats, wide), jnp.float32)
        for row in range(max(tile * wide - ADDENDS, 0) // BLOCK, rows):
            micro, lanes = row // per_micro, pl.ds(row % per_micro * BLOCK, BLOCK)
            values = jnp.concatenate([hidden_ref[micro, :, lanes], cotangent_ref[micro, :, lanes]])
            chosen = place_ref[row * BLOCK : row * BLOCK + BLOCK, :] == slots
            chosen = chosen.astype(jnp.float32).astype(jnp.bfloat16)
            sums += lax.dot_general(values, chosen, dims, preferred_element_type=jnp.float32)
        states = sums[:feats]
        if (tile + 1) * wide in (ALWAYS, sum(LENGTHS)):
            for k, addend in enumerate(addends):
                states = jnp.where(lane == wide - ADDENDS + k, addend, states)
        out[0, :, start : start + wide] = states.astype(jnp.bfloat16)
        out[1, :, start : start + wide] = sums[feats:].astype(jnp.bfloat16)


def counted_first(hidden, cotangent, blocks, loss_mask, gain):
    micro_count, row_count, feats = hidden.shape
    in_vmem = pl.BlockSpec(memory_space=pltpu.VMEM)
    count = micro_count * row_count
    *parts, total = pl.pallas_call(
        counted_kernel,
        out_shape=[jax.ShapeDtypeStruct((2, feats, length), jnp.bfloat16) for length in LENGTHS]
        + [jax.ShapeDtypeStruct((8, 128), jnp.float32)],
        in_specs=[in_vmem] * 5,
        out_specs=[in_vmem] * (len(LENGTHS) + 1),
        scratch_shapes=[pltpu.VMEM((count, 1), jnp.float32)],
        cost_estimate=pl.CostEstimate(flops=2 * feats * count * count, bytes_accessed=8 * feats * count, transcendentals=0),
        name="counted_first",
    )(
        blocks.T,
        loss_mask,
        gain.reshape(1, -1),
        jnp.swapaxes(hidden, 1, 2),
        jnp.swapaxes(cotangent, 1, 2),
    )
    return parts, total[0, 0].astype(jnp.int32)


def gradients_kernel(plan, count, gate_ref, up_ref, down_ref, *refs):
    pieces, out_ref = refs[: len(plan)], refs[len(plan)]
    states, tangent, d_in, inner, in_ref, gain_column, sems = refs[len(plan) + 1 :]
    place_y, place_z = lax.axis_index("y"), lax.axis_index("z")
    feats, units = D // (NY * NZ), down_ref.shape[0]

    def rows_of(back_y, back_z):
        row_y = lax.rem(place_y + 2 * NY - back_y, NY)
        row_z = lax.rem(place_z + 2 * NZ - back_z, NZ)
        return pl.ds(pl.multiple_of((row_y * NZ + row_z) * feats, feats), feats)

    bases = sorted({base for *_, base in plan})
    ends = bases[1:] + [count]
    for tensor, whole in enumerate((states, tangent)):
        for ref, (back_y, back_z, along, base) in sorted(zip(pieces, plan), key=lambda piece: piece[1][-1]):
            sem = sems.at[2 if tensor else bases.index(base)]

            @pl.loop(0, ref.shape[0])
            def _(k):
                if along == "line":
                    line = lax.rem(place_y * NZ + place_z + NY * NZ - k, NY * NZ)
                    rows = rows_of(place_y - line // NZ, place_z - lax.rem(line, NZ))
                else:
                    rows = rows_of(back_y + k, back_z) if along == "y" else rows_of(back_y, back_z + k)
                into = whole.at[rows, pl.ds(base, ref.shape[-1])]
                pltpu.make_async_copy(ref.at[k, tensor], into, sem).start()

    def arrive(ref, sem):
        pltpu.make_async_copy(ref, ref, sem).wait()

    in_ref[:units, :] = gate_ref[...]
    in_ref[units:, :] = up_ref[...]
    wide = SHARE
    height = 256

    def normalize(tile):
        lanes = pl.ds(pl.multiple_of(tile * wide, wide), wide)
        squares = jnp.zeros((8, wide), jnp.float32)
        for top in range(0, D, height):
            x = states[top : top + height, lanes].astype(jnp.float32)
            squares += (x * x).reshape(height // 8, 8, wide).sum(axis=0)
        scale = lax.rsqrt(jnp.sum(squares, axis=0, keepdims=True) / D + 1e-06)
        for top in range(0, D, height):
            x = states[top : top + height, lanes].astype(jnp.float32)
            gain = gain_column[top : top + height, :]
            states[top : top + height, lanes] = (x * scale * gain).astype(jnp.bfloat16)

    for index in reversed(range(len(bases))):
        start, end = bases[index], ends[index]
        arrive(states.at[:, start:end], sems.at[index])
        if end == count:
            addends = states[:, count - 128 : count].astype(jnp.float32)
            lane = lax.broadcasted_iota(jnp.int32, (1, 128), 1)
            gain_column[...] = jnp.sum(jnp.where(lane >= 128 - ADDENDS, addends, 0.0), axis=1, keepdims=True)
    pl.loop(0, count // wide)(normalize)
    arrive(tangent, sems.at[2])

    def forward(lanes):
        dims = (((1,), (0,)), ((), ()))
        pre = lax.dot_general(in_ref[...], states[:, lanes], dims, preferred_element_type=jnp.float32)
        gate_pre, up_pre = pre[:units], pre[units:]
        back = lax.dot_general(down_ref[...], tangent[:, lanes], dims, preferred_element_type=jnp.float32)
        root = 0.7978845608028654
        square = gate_pre * gate_pre
        bent = jnp.tanh(root * gate_pre * (1.0 + 0.044715 * square))
        half = 0.5 * (1.0 + bent)
        activated = gate_pre * half
        slope = half + 0.5 * gate_pre * (1.0 - bent * bent) * root * (1.0 + 3 * 0.044715 * square)
        inner[:, lanes] = (activated * up_pre).astype(jnp.bfloat16)
        d_in[:units, lanes] = (back * up_pre * slope).astype(jnp.bfloat16)
        d_in[units:, lanes] = (back * activated).astype(jnp.bfloat16)

    @pl.loop(0, count // wide)
    def _(tile):
        forward(pl.ds(pl.multiple_of(tile * wide, wide), wide))

    spans = [(start, min(CHUNK, count - start)) for start in range(0, count, CHUNK)]

    def accumulated(left, right, rows):
        total = comp = None
        for start, size in spans:
            term = lax.dot_general(
                left[:, start : start + size],
                right[rows, start : start + size],
                (((1,), (1,)), ((), ())),
                preferred_element_type=jnp.float32,
            )
            if total is None:
                total, comp = term, jnp.zeros_like(term)
                continue
            adjusted = term - comp
            running = total + adjusted
            comp = (running - total) - adjusted
            total = running
        return total

    @pl.loop(0, D // wide)
    def _(tile):
        rows = pl.ds(pl.multiple_of(tile * wide, wide), wide)
        first = accumulated(d_in, states, rows)
        out_ref[tile, 0] = first[:units].astype(jnp.bfloat16)
        out_ref[tile, 1] = first[units:].astype(jnp.bfloat16)
        out_ref[tile, 2] = accumulated(inner, tangent, rows).astype(jnp.bfloat16)


def gradients(pieces, wi_gate, wi_up, wo_weight, count):
    arrays = [array for array, *_ in pieces]
    plan = [where for _, *where in pieces]
    units = wi_gate.shape[0]
    in_vmem = pl.BlockSpec(memory_space=pltpu.VMEM)
    return pl.pallas_call(
        functools.partial(gradients_kernel, plan, count),
        out_shape=jax.ShapeDtypeStruct((D // SHARE, 3, units, SHARE), jnp.bfloat16),
        in_specs=[in_vmem] * 3 + [pl.BlockSpec(memory_space=pl.ANY)] * len(arrays),
        out_specs=in_vmem,
        scratch_shapes=[
            pltpu.VMEM((D, count), jnp.bfloat16),
            pltpu.VMEM((D, count), jnp.bfloat16),
            pltpu.VMEM((2 * units, count), jnp.bfloat16),
            pltpu.VMEM((units, count), jnp.bfloat16),
            pltpu.VMEM((2 * units, D), jnp.bfloat16),
            pltpu.VMEM((D, 1), jnp.float32),
            pltpu.SemaphoreType.DMA((3,)),
        ],
        compiler_params=pltpu.CompilerParams(vmem_limit_bytes=60_000_000),
        cost_estimate=pl.CostEstimate(
            flops=12 * units * D * count, bytes_accessed=8 * D * count, transcendentals=units * count
        ),
        name="gradients",
    )(wi_gate, wi_up, wo_weight, *arrays)


def summed_over_groups(parts, denominator):
    place_x, place_core = lax.axis_index("x"), lax.axis_index("core")
    half = SHARE // 2
    by_core = parts.reshape(2, NX, *parts.shape[1:])
    given = shifted(lax.dynamic_index_in_dim(by_core, 1 - place_core, 0, False), "core", 1)
    pair = lax.dynamic_index_in_dim(by_core, place_core, 0, False).astype(jnp.float32) + given.astype(jnp.float32)

    def due(step):
        return lax.dynamic_index_in_dim(pair, (place_x + step) % NX, 0, False)

    far = due(2).astype(jnp.bfloat16)
    far_ahead = shifted(far[..., :half], "x", 1).astype(jnp.float32)
    far_behind = shifted(far[..., half:], "x", -1).astype(jnp.float32)
    ahead, behind = due(1), due(-1)
    ahead = jnp.concatenate([ahead[..., :half] + far_ahead, ahead[..., half:]], axis=-1)
    behind = jnp.concatenate([behind[..., :half], behind[..., half:] + far_behind], axis=-1)
    from_behind = shifted(ahead.astype(jnp.bfloat16), "x", 1)
    from_ahead = shifted(behind.astype(jnp.bfloat16), "x", -1)
    total = due(0) + from_behind.astype(jnp.float32) + from_ahead.astype(jnp.float32)
    share = (total / denominator).astype(jnp.bfloat16)
    back_1 = shifted(share, "x", 1)
    back_3 = shifted(share, "x", -1)
    back_2 = jnp.concatenate(
        [shifted(back_1[..., :half], "x", 1), shifted(back_3[..., half:], "x", -1)],
        axis=-1,
    )
    own = jnp.stack([share, back_1, back_2, back_3])
    other = shifted(own, "core", 1)
    low = jnp.where(place_core == 0, own, other)
    high = jnp.where(place_core == 0, other, own)
    columns = [
        lax.dynamic_index_in_dim(side, (place_x + NX - x) % NX, 0, False) for side in (low, high) for x in range(NX)
    ]
    return jnp.concatenate(columns, axis=-1).astype(jnp.float32)


def on_device(hidden, gain, cotangent, blocks, loss_mask, wi_gate, wi_up, wo_weight):
    (part_a, part_b, rest), own_total = counted_first(hidden[0], cotangent[0], blocks[0], loss_mask[0], gain)
    pieces = gathered(part_a, part_b)
    totals = sent_to_all(own_total, DP)
    denominator = jnp.maximum(totals.sum(), 1).astype(jnp.float32)
    weights = (wi_gate, wi_up, wo_weight)
    parts = gradients(pieces, *weights, ALWAYS)

    def with_rest(parts):
        size = lax.axis_size(MP)

        def step(k, state):
            block, got = state
            block = lax.ppermute(block, MP, [(i, (i + 1) % size) for i in range(size)])
            return block, lax.dynamic_update_index_in_dim(got, block, k, 0)

        got = jnp.broadcast_to(rest, (size, *rest.shape))
        _, got = lax.fori_loop(1, size, step, (rest, got))
        more = gradients([(got, 0, 0, "line", 0)], *weights, LENGTHS[2])
        return (parts.astype(jnp.float32) + more.astype(jnp.float32)).astype(jnp.bfloat16)

    parts = lax.cond(jnp.max(totals) > ALWAYS - ADDENDS, with_rest, lambda parts: parts, parts)
    return summed_over_groups(parts, denominator)


def solution(mesh):
    torus = Mesh(mesh.devices.reshape(4, 2, NY, NZ), ("x", "core", "y", "z"))

    return jax.shard_map(
        on_device,
        mesh=torus,
        in_specs=(
            P(DP, None, None, MP),
            P(MP),
            P(DP, None, None, MP),
            P(DP, None, None),
            P(DP, None, None),
            P(MP, None),
            P(MP, None),
            P(MP, None),
        ),
        out_specs=P(None, MP, None),
        check_vma=False,
    )
```

```python
import functools

import jax
import jax.numpy as jnp
from jax import lax
from jax.experimental import pallas as pl
from jax.experimental.pallas import tpu as pltpu
from jax.sharding import Mesh
from jax.sharding import PartitionSpec as P


D = 2048
BLOCK = 128
TLEN = 256
DP = ("x", "core")
MP = ("y", "z")
NY = 4
NZ = 8
CHUNK = 512
SHARE = 256
NX = 4
LENGTHS = (640, 896, 768)
ALWAYS = LENGTHS[0] + LENGTHS[1]
ADDENDS = 3
GROUPS_Z = ((7, 3), (2, 5))


def sent_to_all(x, axis):
    devices = lax.axis_size(axis)
    return lax.all_to_all(jnp.broadcast_to(x[None], (devices, *x.shape)), axis, 0, 0, tiled=True)


def shifted(x, axis, step):
    size = lax.axis_size(axis)
    return lax.ppermute(x, axis, [(i, (i + step) % size) for i in range(size)])


def ring(own, axis, cut):
    size = lax.axis_size(axis)
    ahead, behind = own, own
    blocks = {0: own}
    for step in range(1, size // 2):
        ahead = shifted(ahead, axis, 1)
        behind = shifted(behind, axis, -1)
        blocks[step], blocks[size - step] = ahead, behind
    last = size // 2
    blocks[last] = (shifted(ahead[:cut], axis, 1), shifted(behind[cut:], axis, -1))
    return blocks


def joined(blocks, order):
    return jnp.stack([jnp.concatenate(b) if isinstance(b, tuple) else b for b in (blocks[k] for k in order)])


def gathered(part_a, part_b):
    first = part_a.shape[-1]
    pieces = []
    rows_b = ring(part_b, "z", 1)
    joined_a = joined(ring(part_a, "y", 1), range(NY))
    for back_z, got in ring(joined_a, "z", NY // 2).items():
        if isinstance(got, tuple):
            pieces.append((got[0], 0, back_z, "y", 0))
            pieces.append((got[1], NY // 2, back_z, "y", 0))
        else:
            pieces.append((got, 0, back_z, "y", 0))
    for (least, many), cut in zip(GROUPS_Z, (1, 3)):
        group = joined(rows_b, [(least + k) % NZ for k in range(many)])
        for back_y, got in ring(group, "y", cut).items():
            if isinstance(got, tuple):
                pieces.append((got[0], back_y, least, "z", first))
                pieces.append((got[1], back_y, least + cut, "z", first))
            else:
                pieces.append((got, back_y, least, "z", first))
    return pieces


def turned(rows, out_ref):
    square = jnp.concatenate([rows, jnp.zeros((128 - rows.shape[0], 128), rows.dtype)]).T
    for k in range(rows.shape[0]):
        out_ref[k * 128 : k * 128 + 128, :] = square[:, k : k + 1]


def counted_kernel(blocks_ref, mask_ref, gain_ref, hidden_ref, cotangent_ref, *refs):
    outs, total_ref, place_ref = refs[:-2], refs[-2], refs[-1]
    micro_count, feats, row_count = hidden_ref.shape
    per_micro, per_sequence = row_count // BLOCK, TLEN // BLOCK
    rows = micro_count * per_micro
    weight = []
    for row in range(rows):
        micro, block = row // per_micro, row % per_micro
        sequence = block // per_sequence
        used = blocks_ref[sequence : sequence + 1, micro : micro + 1] > block % per_sequence
        mask = mask_ref[micro : micro + 1, block * BLOCK : block * BLOCK + BLOCK]
        weight.append(jnp.where(used, mask, 0))
    weight = jnp.concatenate(weight).astype(jnp.float32)
    narrow = weight.astype(jnp.bfloat16)
    dims = (((1,), (0,)), ((), ()))

    def triangle(size, strict):
        one, two = (lax.broadcasted_iota(jnp.int32, (size, size), k) for k in (0, 1))
        return (one > two if strict else one <= two).astype(jnp.float32).astype(jnp.bfloat16)

    within = lax.dot_general(narrow, triangle(BLOCK, False), dims, preferred_element_type=jnp.float32)
    before = lax.dot_general(triangle(rows, True), narrow, dims, preferred_element_type=jnp.float32)
    rank = within + jnp.sum(before, axis=1, keepdims=True) - 1.0
    slot = jnp.where(rank < ALWAYS - ADDENDS, rank, rank + ADDENDS)
    turned(jnp.where(weight > 0, slot, -1.0), place_ref)
    total_ref[...] = jnp.broadcast_to(jnp.sum(weight), total_ref.shape)
    one, two = (lax.broadcasted_iota(jnp.int32, (feats, feats), k) for k in (0, 1))
    left = jnp.sum(jnp.where(one == two, gain_ref[...], 0.0), axis=1, keepdims=True)
    addends = []
    for _ in range(ADDENDS):
        addends.append(left.astype(jnp.bfloat16).astype(jnp.float32))
        left = left - addends[-1]
    wide = SHARE
    into = [(out, start) for out in outs for start in range(0, out.shape[2], BLOCK)]
    for tile in range(sum(LENGTHS) // wide):
        lane = lax.broadcasted_iota(jnp.int32, (1, wide), 1)
        slots = (lane + tile * wide).astype(jnp.float32)
        sums = jnp.zeros((2 * feats, wide), jnp.float32)
        for row in range(max(tile * wide - ADDENDS, 0) // BLOCK, rows):
            micro, lanes = row // per_micro, pl.ds(row % per_micro * BLOCK, BLOCK)
            values = jnp.concatenate([hidden_ref[micro, :, lanes], cotangent_ref[micro, :, lanes]])
            chosen = place_ref[row * BLOCK : row * BLOCK + BLOCK, :] == slots
            chosen = chosen.astype(jnp.float32).astype(jnp.bfloat16)
            sums += lax.dot_general(values, chosen, dims, preferred_element_type=jnp.float32)
        states = sums[:feats]
        if (tile + 1) * wide in (ALWAYS, sum(LENGTHS)):
            for k, addend in enumerate(addends):
                states = jnp.where(lane == wide - ADDENDS + k, addend, states)
        for k in range(wide // BLOCK):
            out, start = into[tile * (wide // BLOCK) + k]
            lanes, among = pl.ds(start, BLOCK), slice(k * BLOCK, k * BLOCK + BLOCK)
            out[0, :, lanes] = states[:, among].astype(jnp.bfloat16)
            out[1, :, lanes] = sums[feats:, among].astype(jnp.bfloat16)


def counted_first(hidden, cotangent, blocks, loss_mask, gain):
    micro_count, row_count, feats = hidden.shape
    in_vmem = pl.BlockSpec(memory_space=pltpu.VMEM)
    count = micro_count * row_count
    *parts, total = pl.pallas_call(
        counted_kernel,
        out_shape=[jax.ShapeDtypeStruct((2, feats, length), jnp.bfloat16) for length in LENGTHS]
        + [jax.ShapeDtypeStruct((8, 128), jnp.float32)],
        in_specs=[in_vmem] * 5,
        out_specs=[in_vmem] * (len(LENGTHS) + 1),
        scratch_shapes=[pltpu.VMEM((count, 1), jnp.float32)],
        cost_estimate=pl.CostEstimate(flops=2 * feats * count * count, bytes_accessed=8 * feats * count, transcendentals=0),
        name="counted_first",
    )(
        blocks.T,
        loss_mask,
        gain.reshape(1, -1),
        jnp.swapaxes(hidden, 1, 2),
        jnp.swapaxes(cotangent, 1, 2),
    )
    return parts, total[0, 0].astype(jnp.int32)


def gradients_kernel(plan, count, gate_ref, up_ref, down_ref, *refs):
    pieces, out_ref = refs[: len(plan)], refs[len(plan)]
    states, tangent, d_in, inner, in_ref, gain_column, sems = refs[len(plan) + 1 :]
    place_y, place_z = lax.axis_index("y"), lax.axis_index("z")
    feats, units = D // (NY * NZ), down_ref.shape[0]

    def rows_of(back_y, back_z):
        row_y = lax.rem(place_y + 2 * NY - back_y, NY)
        row_z = lax.rem(place_z + 2 * NZ - back_z, NZ)
        return pl.ds(pl.multiple_of((row_y * NZ + row_z) * feats, feats), feats)

    bases = sorted({base for *_, base in plan})
    ends = bases[1:] + [count]
    for tensor, whole in enumerate((states, tangent)):
        for ref, (back_y, back_z, along, base) in sorted(zip(pieces, plan), key=lambda piece: piece[1][-1]):
            sem = sems.at[2 if tensor else bases.index(base)]

            @pl.loop(0, ref.shape[0])
            def _(k):
                if along == "line":
                    line = lax.rem(place_y * NZ + place_z + NY * NZ - k, NY * NZ)
                    rows = rows_of(place_y - line // NZ, place_z - lax.rem(line, NZ))
                else:
                    rows = rows_of(back_y + k, back_z) if along == "y" else rows_of(back_y, back_z + k)
                into = whole.at[rows, pl.ds(base, ref.shape[-1])]
                pltpu.make_async_copy(ref.at[k, tensor], into, sem).start()

    def arrive(ref, sem):
        pltpu.make_async_copy(ref, ref, sem).wait()

    in_ref[:units, :] = gate_ref[...]
    in_ref[units:, :] = up_ref[...]
    wide = SHARE
    height = 256

    def normalize(tile):
        lanes = pl.ds(pl.multiple_of(tile * wide, wide), wide)
        squares = jnp.zeros((8, wide), jnp.float32)
        for top in range(0, D, height):
            x = states[top : top + height, lanes].astype(jnp.float32)
            squares += (x * x).reshape(height // 8, 8, wide).sum(axis=0)
        scale = lax.rsqrt(jnp.sum(squares, axis=0, keepdims=True) / D + 1e-06)
        for top in range(0, D, height):
            x = states[top : top + height, lanes].astype(jnp.float32)
            gain = gain_column[top : top + height, :]
            states[top : top + height, lanes] = (x * scale * gain).astype(jnp.bfloat16)

    for index in reversed(range(len(bases))):
        start, end = bases[index], ends[index]
        arrive(states.at[:, start:end], sems.at[index])
        if end == count:
            addends = states[:, count - 128 : count].astype(jnp.float32)
            lane = lax.broadcasted_iota(jnp.int32, (1, 128), 1)
            gain_column[...] = jnp.sum(jnp.where(lane >= 128 - ADDENDS, addends, 0.0), axis=1, keepdims=True)
    pl.loop(0, count // wide)(normalize)
    arrive(tangent, sems.at[2])

    def forward(lanes):
        dims = (((1,), (0,)), ((), ()))
        pre = lax.dot_general(in_ref[...], states[:, lanes], dims, preferred_element_type=jnp.float32)
        gate_pre, up_pre = pre[:units], pre[units:]
        back = lax.dot_general(down_ref[...], tangent[:, lanes], dims, preferred_element_type=jnp.float32)
        root = 0.7978845608028654
        square = gate_pre * gate_pre
        bent = jnp.tanh(root * gate_pre * (1.0 + 0.044715 * square))
        half = 0.5 * (1.0 + bent)
        activated = gate_pre * half
        slope = half + 0.5 * gate_pre * (1.0 - bent * bent) * root * (1.0 + 3 * 0.044715 * square)
        inner[:, lanes] = (activated * up_pre).astype(jnp.bfloat16)
        d_in[:units, lanes] = (back * up_pre * slope).astype(jnp.bfloat16)
        d_in[units:, lanes] = (back * activated).astype(jnp.bfloat16)

    @pl.loop(0, count // wide)
    def _(tile):
        forward(pl.ds(pl.multiple_of(tile * wide, wide), wide))

    spans = [(start, min(CHUNK, count - start)) for start in range(0, count, CHUNK)]

    def accumulated(left, right, rows):
        total = comp = None
        for start, size in spans:
            term = lax.dot_general(
                left[:, start : start + size],
                right[rows, start : start + size],
                (((1,), (1,)), ((), ())),
                preferred_element_type=jnp.float32,
            )
            if total is None:
                total, comp = term, jnp.zeros_like(term)
                continue
            adjusted = term - comp
            running = total + adjusted
            comp = (running - total) - adjusted
            total = running
        return total

    @pl.loop(0, D // wide)
    def _(tile):
        rows = pl.ds(pl.multiple_of(tile * wide, wide), wide)
        first = accumulated(d_in, states, rows)
        out_ref[tile, 0] = first[:units].astype(jnp.bfloat16)
        out_ref[tile, 1] = first[units:].astype(jnp.bfloat16)
        out_ref[tile, 2] = accumulated(inner, tangent, rows).astype(jnp.bfloat16)


def gradients(pieces, wi_gate, wi_up, wo_weight, count):
    arrays = [array for array, *_ in pieces]
    plan = [where for _, *where in pieces]
    units = wi_gate.shape[0]
    in_vmem = pl.BlockSpec(memory_space=pltpu.VMEM)
    return pl.pallas_call(
        functools.partial(gradients_kernel, plan, count),
        out_shape=jax.ShapeDtypeStruct((D // SHARE, 3, units, SHARE), jnp.bfloat16),
        in_specs=[in_vmem] * 3 + [pl.BlockSpec(memory_space=pl.ANY)] * len(arrays),
        out_specs=in_vmem,
        scratch_shapes=[
            pltpu.VMEM((D, count), jnp.bfloat16),
            pltpu.VMEM((D, count), jnp.bfloat16),
            pltpu.VMEM((2 * units, count), jnp.bfloat16),
            pltpu.VMEM((units, count), jnp.bfloat16),
            pltpu.VMEM((2 * units, D), jnp.bfloat16),
            pltpu.VMEM((D, 1), jnp.float32),
            pltpu.SemaphoreType.DMA((3,)),
        ],
        compiler_params=pltpu.CompilerParams(vmem_limit_bytes=60_000_000),
        cost_estimate=pl.CostEstimate(
            flops=12 * units * D * count, bytes_accessed=8 * D * count, transcendentals=units * count
        ),
        name="gradients",
    )(wi_gate, wi_up, wo_weight, *arrays)


def summed_over_groups(parts, denominator):
    place_x, place_core = lax.axis_index("x"), lax.axis_index("core")
    half = SHARE // 2
    by_core = parts.reshape(2, NX, *parts.shape[1:])
    given = shifted(lax.dynamic_index_in_dim(by_core, 1 - place_core, 0, False), "core", 1)
    pair = lax.dynamic_index_in_dim(by_core, place_core, 0, False).astype(jnp.float32) + given.astype(jnp.float32)

    def due(step):
        return lax.dynamic_index_in_dim(pair, (place_x + step) % NX, 0, False)

    far = due(2).astype(jnp.bfloat16)
    far_ahead = shifted(far[..., :half], "x", 1).astype(jnp.float32)
    far_behind = shifted(far[..., half:], "x", -1).astype(jnp.float32)
    ahead, behind = due(1), due(-1)
    ahead = jnp.concatenate([ahead[..., :half] + far_ahead, ahead[..., half:]], axis=-1)
    behind = jnp.concatenate([behind[..., :half], behind[..., half:] + far_behind], axis=-1)
    from_behind = shifted(ahead.astype(jnp.bfloat16), "x", 1)
    from_ahead = shifted(behind.astype(jnp.bfloat16), "x", -1)
    total = due(0) + from_behind.astype(jnp.float32) + from_ahead.astype(jnp.float32)
    share = (total / denominator).astype(jnp.bfloat16)
    back_1 = shifted(share, "x", 1)
    back_3 = shifted(share, "x", -1)
    back_2 = jnp.concatenate(
        [shifted(back_1[..., :half], "x", 1), shifted(back_3[..., half:], "x", -1)],
        axis=-1,
    )
    own = jnp.stack([share, back_1, back_2, back_3])
    other = shifted(own, "core", 1)
    low = jnp.where(place_core == 0, own, other)
    high = jnp.where(place_core == 0, other, own)
    columns = [
        lax.dynamic_index_in_dim(side, (place_x + NX - x) % NX, 0, False) for side in (low, high) for x in range(NX)
    ]
    return jnp.concatenate(columns, axis=-1).astype(jnp.float32)


def on_device(hidden, gain, cotangent, blocks, loss_mask, wi_gate, wi_up, wo_weight):
    (part_a, part_b, rest), own_total = counted_first(hidden[0], cotangent[0], blocks[0], loss_mask[0], gain)
    pieces = gathered(part_a, part_b)
    totals = sent_to_all(own_total, DP)
    denominator = jnp.maximum(totals.sum(), 1).astype(jnp.float32)
    weights = (wi_gate, wi_up, wo_weight)
    parts = gradients(pieces, *weights, ALWAYS)

    def with_rest(parts):
        size = lax.axis_size(MP)

        def step(k, state):
            block, got = state
            block = lax.ppermute(block, MP, [(i, (i + 1) % size) for i in range(size)])
            return block, lax.dynamic_update_index_in_dim(got, block, k, 0)

        got = jnp.broadcast_to(rest, (size, *rest.shape))
        _, got = lax.fori_loop(1, size, step, (rest, got))
        more = gradients([(got, 0, 0, "line", 0)], *weights, LENGTHS[2])
        return (parts.astype(jnp.float32) + more.astype(jnp.float32)).astype(jnp.bfloat16)

    parts = lax.cond(jnp.max(totals) > ALWAYS - ADDENDS, with_rest, lambda parts: parts, parts)
    return summed_over_groups(parts, denominator)


def solution(mesh):
    torus = Mesh(mesh.devices.reshape(4, 2, NY, NZ), ("x", "core", "y", "z"))

    return jax.shard_map(
        on_device,
        mesh=torus,
        in_specs=(
            P(DP, None, None, MP),
            P(MP),
            P(DP, None, None, MP),
            P(DP, None, None),
            P(DP, None, None),
            P(MP, None),
            P(MP, None),
            P(MP, None),
        ),
        out_specs=P(None, MP, None),
        check_vma=False,
    )
```
